32 devices in a mesh: data: 4 (over z), stage: 8 (over y, x, core).
Axes of the slice: x: 2, y: 2, z: 4, core: 2. Of those that a mesh axis runs over, the one named last changes fastest.
Arguments:
- act_in: bfloat16 [24, 128, 16, 256], P(None, 'data')
- cot_out: bfloat16 [24, 128, 16, 256], P(None, 'data')
- w_gate: bfloat16 [2, 8, 256, 1024], P(None, 'stage', 'data')
- w_in: bfloat16 [2, 8, 256, 1024], P(None, 'stage', 'data')
- w_out: bfloat16 [2, 8, 1024, 256], P(None, 'stage', 'data')
Outputs:
- output 1: bfloat16 [24, 128, 16, 256], P(None, 'data')
- output 2: float32 [2, 8, 256, 1024], P(None, 'stage', 'data')
- output 3: float32 [2, 8, 256, 1024], P(None, 'stage', 'data')
- output 4: float32 [2, 8, 1024, 256], P(None, 'stage', 'data')
All inputs are finite; a program needn't handle non-finite values.
Results may differ from the reference program's by a relative error of at most 0.02.
Values are sent between devices in bfloat16 or wider.
A program may use at most 1 GiB of HBM per device.

```python
import jax
import jax.numpy as jnp
from jax import lax

DMODEL = 256
FFN_DIM = 1024
STAGES = 8
NUM_MICRO = 24
BATCH_ROWS = 128
SEQLEN = 16
NORM_EPS = 1e-6


def setup_inputs(seed: int = 0) -> dict:
    sub_keys = jax.random.split(jax.random.key(seed), 5)
    act_shape = (NUM_MICRO, BATCH_ROWS, SEQLEN, DMODEL)
    up_shape = (2, STAGES, DMODEL, FFN_DIM)
    down_shape = (2, STAGES, FFN_DIM, DMODEL)
    act_in = jax.random.normal(sub_keys[0], act_shape, jnp.float32)
    cot_out = jax.random.normal(sub_keys[1], act_shape, jnp.float32)
    w_gate = jax.random.normal(sub_keys[2], up_shape, jnp.float32) * DMODEL ** -0.5
    w_in = jax.random.normal(sub_keys[3], up_shape, jnp.float32) * DMODEL ** -0.5
    w_out = jax.random.normal(sub_keys[4], down_shape, jnp.float32) * FFN_DIM ** -0.5
    return dict(act_in=act_in.astype(jnp.bfloat16), cot_out=cot_out.astype(jnp.bfloat16), w_gate=w_gate.astype(jnp.bfloat16), w_in=w_in.astype(jnp.bfloat16), w_out=w_out.astype(jnp.bfloat16))


def layer_forward(rows_in, gate_w, lin_w, proj_w):
    rows_f32 = rows_in.astype(jnp.float32)
    inv_rms = lax.rsqrt(jnp.mean(rows_f32 * rows_f32, axis=-1, keepdims=True) + NORM_EPS)
    normed = (rows_f32 * inv_rms).astype(jnp.bfloat16)
    gate_pre = jnp.dot(normed, gate_w, preferred_element_type=jnp.float32)
    lin_pre = jnp.dot(normed, lin_w, preferred_element_type=jnp.float32)
    gate_act = gate_pre * jax.nn.sigmoid(gate_pre)
    hidden = (gate_act * lin_pre).astype(jnp.bfloat16)
    proj_out = jnp.dot(hidden, proj_w, preferred_element_type=jnp.float32)
    return (rows_f32 + proj_out).astype(jnp.bfloat16)


def layer_backward(rows_in, grad_rows, gate_w, lin_w, proj_w):
    rows_f32 = rows_in.astype(jnp.float32)
    inv_rms = lax.rsqrt(jnp.mean(rows_f32 * rows_f32, axis=-1, keepdims=True) + NORM_EPS)
    scaled = rows_f32 * inv_rms
    normed = scaled.astype(jnp.bfloat16)
    gate_pre = jnp.dot(normed, gate_w, preferred_element_type=jnp.float32)
    lin_pre = jnp.dot(normed, lin_w, preferred_element_type=jnp.float32)
    gate_sig = jax.nn.sigmoid(gate_pre)
    gate_act = gate_pre * gate_sig
    hidden = (gate_act * lin_pre).astype(jnp.bfloat16)
    grad_proj = jnp.dot(hidden.T, grad_rows, preferred_element_type=jnp.float32)
    grad_hidden = jnp.dot(grad_rows, proj_w.T, preferred_element_type=jnp.float32)
    d_gate = (grad_hidden * lin_pre * gate_sig * (1.0 + gate_pre * (1.0 - gate_sig))).astype(jnp.bfloat16)
    d_lin = (grad_hidden * gate_act).astype(jnp.bfloat16)
    grad_gate = jnp.dot(normed.T, d_gate, preferred_element_type=jnp.float32)
    grad_lin = jnp.dot(normed.T, d_lin, preferred_element_type=jnp.float32)
    grad_norm = jnp.dot(d_gate, gate_w.T, preferred_element_type=jnp.float32) + jnp.dot(d_lin, lin_w.T, preferred_element_type=jnp.float32)
    grad_in = grad_rows.astype(jnp.float32) + inv_rms * (grad_norm - scaled * jnp.mean(grad_norm * scaled, axis=-1, keepdims=True))
    return grad_in.astype(jnp.bfloat16), grad_gate, grad_lin, grad_proj


def reference(act_in, cot_out, w_gate, w_in, w_out):
    layers = 2 * STAGES
    tok_rows = BATCH_ROWS * SEQLEN
    gate_stack = w_gate.reshape(layers, DMODEL, FFN_DIM)
    lin_stack = w_in.reshape(layers, DMODEL, FFN_DIM)
    proj_stack = w_out.reshape(layers, FFN_DIM, DMODEL)
    act_micro = act_in.reshape(NUM_MICRO, tok_rows, DMODEL)
    cot_micro = cot_out.reshape(NUM_MICRO, tok_rows, DMODEL)

    def fwd_body(rows_in, weights):
        return layer_forward(rows_in, weights[0], weights[1], weights[2]), rows_in

    def bwd_body(grad_rows, packed):
        gate_w, lin_w, proj_w, rows_in = packed
        grad_in, grad_g, grad_l, grad_p = layer_backward(rows_in, grad_rows, gate_w, lin_w, proj_w)
        return grad_in, (grad_g, grad_l, grad_p)

    def micro_step(totals, pair):
        act_rows, cot_rows = pair
        last_rows, saved_in = lax.scan(fwd_body, act_rows, (gate_stack, lin_stack, proj_stack))
        grad_x, per_layer = lax.scan(bwd_body, cot_rows, (gate_stack, lin_stack, proj_stack, saved_in), reverse=True)
        new_totals = tuple(running + layer_part for running, layer_part in zip(totals, per_layer))
        return new_totals, grad_x

    zero_up = jnp.zeros((layers, DMODEL, FFN_DIM), jnp.float32)
    zero_down = jnp.zeros((layers, FFN_DIM, DMODEL), jnp.float32)
    totals, grad_act = lax.scan(micro_step, (zero_up, zero_up, zero_down), (act_micro, cot_micro))
    return (grad_act.reshape(NUM_MICRO, BATCH_ROWS, SEQLEN, DMODEL), totals[0].reshape(2, STAGES, DMODEL, FFN_DIM), totals[1].reshape(2, STAGES, DMODEL, FFN_DIM), totals[2].reshape(2, STAGES, FFN_DIM, DMODEL))
```

```python
import jax
import jax.numpy as jnp
from jax import lax
from jax.sharding import PartitionSpec as P

NORM_EPS = 1e-6
GRP = ("stage", "data")


def dot_rows(left, right):
    return lax.dot_general(left, right, (((0,), (0,)), ((), ())), preferred_element_type=jnp.float32)


def dot_cols(left, right):
    return lax.dot_general(left, right, (((1,), (1,)), ((), ())), preferred_element_type=jnp.float32)


def dot_f32(left, right):
    return jnp.dot(left, right, preferred_element_type=jnp.float32)


def block_forward(rows, gate_w, lin_w, proj_w):
    h = rows.astype(jnp.float32)
    r = lax.rsqrt(jnp.mean(h * h, axis=-1, keepdims=True) + NORM_EPS)
    n = (h * r).astype(jnp.bfloat16)
    a = dot_f32(n, gate_w)
    b = dot_f32(n, lin_w)
    u = (a * jax.nn.sigmoid(a) * b).astype(jnp.bfloat16)
    return (h + dot_f32(u, proj_w)).astype(jnp.bfloat16)


def block_backward(rows, e, gate_w, lin_w, proj_w):
    h = rows.astype(jnp.float32)
    r = lax.rsqrt(jnp.mean(h * h, axis=-1, keepdims=True) + NORM_EPS)
    hr = h * r
    n = hr.astype(jnp.bfloat16)
    a = dot_f32(n, gate_w)
    b = dot_f32(n, lin_w)
    s = jax.nn.sigmoid(a)
    act = a * s
    u = (act * b).astype(jnp.bfloat16)
    d_out = dot_rows(u, e)
    t = dot_cols(e, proj_w)
    da = (t * b * s * (1.0 + a * (1.0 - s))).astype(jnp.bfloat16)
    db = (t * act).astype(jnp.bfloat16)
    d_gate = dot_rows(n, da)
    d_in = dot_rows(n, db)
    q = dot_cols(da, gate_w) + dot_cols(db, lin_w)
    g = e.astype(jnp.float32) + r * (q - hr * jnp.mean(q * hr, axis=-1, keepdims=True))
    return g.astype(jnp.bfloat16), d_gate, d_in, d_out


def solution(mesh):
    n_stage = mesh.shape["stage"]
    act_spec = P(None, "data", None, None)
    w_spec = P(None, "stage", "data", None)

    def body(act_in, cot_out, w_gate, w_in, w_out):
        n_micro, n_seq, n_tok, width = act_in.shape
        n_v = w_gate.shape[0]
        own = n_micro // n_stage
        stage = lax.axis_index("stage")
        h = lax.dynamic_slice_in_dim(act_in, stage * own, own, 0).reshape(-1, width)
        e = lax.dynamic_slice_in_dim(cot_out, stage * own, own, 0).reshape(-1, width)

        def whole(w, v):
            full = lax.all_gather(w[v, 0], GRP, axis=0, tiled=True)
            return full.reshape(n_stage, -1, w.shape[3])

        weights = [tuple(whole(w, v) for w in (w_gate, w_in, w_out)) for v in range(n_v)]
        saved = []
        for v in range(n_v):
            for p in range(n_stage):
                saved.append(h)
                h = block_forward(h, *(w[p] for w in weights[v]))
        grads = [None] * n_v
        for v in reversed(range(n_v)):
            parts = [None] * n_stage
            for p in reversed(range(n_stage)):
                e, *parts[p] = block_backward(saved[v * n_stage + p], e, *(w[p] for w in weights[v]))
            grads[v] = []
            for k in range(3):
                stacked = jnp.concatenate([parts[p][k] for p in range(n_stage)], axis=0)
                grads[v].append(lax.psum_scatter(stacked, GRP, scatter_dimension=0, tiled=True))
        grad_act = lax.all_gather(e.reshape(own, n_seq, n_tok, width), "stage", axis=0, tiled=True)
        outs = [jnp.stack([grads[v][k] for v in range(n_v)])[:, None] for k in range(3)]
        return grad_act, *outs

    return jax.shard_map(body, mesh=mesh, in_specs=(act_spec, act_spec, w_spec, w_spec, w_spec), out_specs=(act_spec, w_spec, w_spec, w_spec), check_vma=False)
```

```python
import functools

import jax
import jax.numpy as jnp
from jax import lax
from jax.experimental import pallas as pl
from jax.experimental.pallas import tpu as pltpu
from jax.sharding import PartitionSpec as P

NORM_EPS = 1e-6
MESH = pl.DeviceIdType.MESH
SLOTS = 8
FWD_LEAD = 7
BWD_DRAIN = 8
LANE, WIDE, HALF = 128, 256, 512
PIECE, SUB = 64, 32
F32 = jnp.float32
BF16 = jnp.bfloat16


class Place:
    def __init__(self):
        self.z, self.s = lax.axis_index("data"), lax.axis_index("stage")
        self.core, self.x, self.y = self.s % 2, (self.s // 2) % 2, self.s // 4
        self.zn, self.zf = self.z % 2, self.z // 2
        self.to_x = (self.z, self.s + 2 - 4 * self.x)
        self.to_y = (self.z, self.s + 4 - 8 * self.y)
        self.to_core = (self.z, self.s + 1 - 2 * self.core)
        self.to_zn = (self.z + 1 - 2 * self.zn, self.s)
        self.to_zf = (self.z + 2 - 4 * self.zf, self.s)


def col(start, size):
    return pl.ds(pl.multiple_of(start, LANE), size)


def narrow(core, hi, lo):
    return HALF * core + WIDE * hi + LANE * lo


def remote(src, dst, ssem, rsem, to):
    return pltpu.make_async_remote_copy(src_ref=src, dst_ref=dst, send_sem=ssem, recv_sem=rsem, device_id=to, device_id_type=MESH)


def wait_bytes(ref, sem):
    pltpu.make_async_copy(ref, ref, sem).wait()


def enter(here, n_stage):
    barrier = pltpu.get_barrier_semaphore()
    peers = [(here.z, (here.s + k) % n_stage) for k in range(1, n_stage)] + [here.to_zn, here.to_zf]
    for peer in peers:
        pl.semaphore_signal(barrier, inc=1, device_id=peer, device_id_type=MESH)
    pl.semaphore_wait(barrier, len(peers))


def mat_rows(left, right):
    return lax.dot_general(left, right, (((0,), (0,)), ((), ())), preferred_element_type=F32)


def mat_cols(left, right):
    return lax.dot_general(left, right, (((1,), (1,)), ((), ())), preferred_element_type=F32)


def mat(left, right):
    return jnp.dot(left, right, preferred_element_type=F32)


def square(w_ref, at, m, k):
    return w_ref[at, m, :, :, :, WIDE * k : WIDE * k + WIDE].reshape(WIDE, WIDE)


def out_square(w_ref, at, k):
    return jnp.concatenate([w_ref[at, 2, k // 2, k % 2, :, WIDE * j : WIDE * j + WIDE] for j in range(4)], axis=0)


def fwd_kernel(n_stage, act, wg, wi, wo, w_all, h_all, w, h, s0, r0, ssem, rsem, lsem, hsem, wsem):
    here = Place()
    z, s, zn, zf = here.z, here.s, here.zn, here.zf
    n_block = w.shape[0]
    n_v = n_block // n_stage
    rows = h.shape[1]
    tile = min(WIDE, rows // 2)
    c_g, c_i = narrow(here.core, here.x, here.y), narrow(here.core, here.y, here.x)
    c_x, c_y, c_c = narrow(here.core, here.x, 0), narrow(here.core, here.y, 0), narrow(here.core, 0, 0)

    enter(here, n_stage)
    load = pltpu.make_async_copy(act.at[s], h.at[0], lsem)
    load.start()

    def scatter(v, k):
        q = (s + k) % n_stage
        core, x, y = q % 2, (q // 2) % 2, q // 4
        d_g, d_i = narrow(core, x, y), narrow(core, y, x)
        c = v * n_stage + s
        moves = (
            (wg.at[v, 0, :, col(d_g, LANE)], w.at[c, 0, zf, zn, :, col(d_g, LANE)]),
            (wi.at[v, 0, :, col(d_i, LANE)], w.at[c, 1, zf, zn, :, col(d_i, LANE)]),
            (wo.at[v, 0, pl.ds(pl.multiple_of(PIECE * (2 * core + x), SUB), SUB), col(LANE * y, LANE)], w.at[c, 2, zf, zn, 0:SUB, col(d_g, LANE)]),
            (wo.at[v, 0, pl.ds(pl.multiple_of(PIECE * (2 * core + y) + SUB, SUB), SUB), col(LANE * x, LANE)], w.at[c, 2, zf, zn, SUB:PIECE, col(d_i, LANE)]),
        )
        for src, dst in moves:
            if k == 0:
                pltpu.make_async_copy(src, dst, r0.at[c]).start()
            else:
                remote(src, dst, s0.at[v], r0.at[c], (z, q)).start()

    for v in range(n_v):
        for k in range(n_stage):
            scatter(v, k)

    def parts(phase, c):
        if phase == 1:
            return (
                (w.at[c, 0, zf, zn, :, col(c_g, LANE)], here.to_zf),
                (w.at[c, 1, zf, zn, :, col(c_i, LANE)], here.to_zf),
                (w.at[c, 2, zf, zn, 0:SUB, col(c_g, LANE)], here.to_zf),
                (w.at[c, 2, zf, zn, SUB:PIECE, col(c_i, LANE)], here.to_zf),
            )
        if phase == 2:
            return (
                (w.at[c, 0, :, zn, :, col(c_g, LANE)], here.to_zn),
                (w.at[c, 1, :, zn, :, col(c_i, LANE)], here.to_zn),
                (w.at[c, 2, :, zn, 0:SUB, col(c_g, LANE)], here.to_y),
                (w.at[c, 2, :, zn, SUB:PIECE, col(c_i, LANE)], here.to_x),
            )
        if phase == 3:
            return (
                (w.at[c, 0, :, :, :, col(c_g, LANE)], here.to_y),
                (w.at[c, 1, :, :, :, col(c_i, LANE)], here.to_x),
                (w.at[c, 2, :, zn, 0:SUB, col(c_x, WIDE)], here.to_x),
                (w.at[c, 2, :, zn, SUB:PIECE, col(c_y, WIDE)], here.to_y),
            )
        if phase == 4:
            return (
                (w.at[c, 0, :, :, :, col(c_x, WIDE)], here.to_x),
                (w.at[c, 1, :, :, :, col(c_y, WIDE)], here.to_y),
                (w.at[c, 2, :, zn, :, col(c_c, HALF)], here.to_zn),
            )
        return ((w.at[c, :, :, :, :, col(c_c, HALF)], here.to_core),)

    def total(phase, c):
        if phase == 1:
            return w.at[c, :, 0, 0, :, 0:LANE]
        if phase == 2:
            return w.at[c, :, :, 0, :, 0:LANE]
        return w.at[c, :, :, :, :, 0 : {3: LANE, 4: WIDE, 5: HALF}[phase]]

    def arrived(phase, c):
        if phase == 0:
            wait_bytes(total(1, c), r0.at[c])
        else:
            slot = c % SLOTS
            wait_bytes(total(phase, c), rsem.at[phase - 1, slot])
            wait_bytes(total(phase, c), ssem.at[phase - 1, slot])

    def advance(phase, c):
        @pl.when((c >= 0) & (c < n_block))
        def _():
            arrived(phase - 1, c)
            slot = c % SLOTS
            for ref, to in parts(phase, c):
                remote(ref, ref, ssem.at[phase - 1, slot], rsem.at[phase - 1, slot], to).start()

    def one_tile(c, i):
        at = pl.ds(pl.multiple_of(i * tile, tile), tile)
        x32 = h[c, at, :].astype(F32)
        inv = lax.rsqrt(jnp.mean(x32 * x32, axis=-1, keepdims=True) + NORM_EPS)
        n = (x32 * inv).astype(BF16)
        acc = x32
        for k in range(4):
            a = mat(n, square(w, c, 0, k))
            b = mat(n, square(w, c, 1, k))
            u = (a * jax.nn.sigmoid(a) * b).astype(BF16)
            acc += mat(u, out_square(w, c, k))
        h[c + 1, at, :] = acc.astype(BF16)

    per_half = rows // tile // 2

    def half_step(i, carry):
        c = i // 2 - FWD_LEAD
        second = i % 2 == 1

        @pl.when(i % 2 == 0)
        def _():
            advance(4, c + 2)
            advance(2, c + 5)

            @pl.when(c == 0)
            def _():
                load.wait()

            @pl.when(c >= 0)
            def _():
                arrived(5, c)

        @pl.when(second)
        def _():
            advance(5, c + 1)
            advance(3, c + 4)
            advance(1, c + 7)

            @pl.when(c >= 0)
            def _():
                pltpu.make_async_copy(w.at[c], w_all.at[c], wsem.at[c]).start()
                pltpu.make_async_copy(h.at[c], h_all.at[c], hsem.at[c]).start()

        @pl.when((c >= 0) & (c < n_block - 1))
        def _():
            def body(j, carry):
                one_tile(c, (i % 2) * per_half + j)
                return carry

            lax.fori_loop(0, per_half, body, 0)

        return carry

    lax.fori_loop(0, 2 * (n_block + FWD_LEAD), half_step, 0)
    for v in range(n_v):
        wait_bytes(w.at[0, :, 0, 0, :, 0 : LANE * (n_stage - 1)], s0.at[v])

    def drain(c, carry):
        pltpu.make_async_copy(w.at[c], w_all.at[c], wsem.at[c]).wait()
        pltpu.make_async_copy(h.at[c], h_all.at[c], hsem.at[c]).wait()
        return carry

    lax.fori_loop(0, n_block, drain, 0)


def bwd_kernel(n_stage, cot, w_all, h_all, gg, gi, go, ga, w, h, e, g, x1, x2g, x2i, x2o, x3g, x3i, x3a, x3b, x4g, x4i, x4a, x4b, x5g, x5i, x5a, x5b, fg, fi, fa, fb, ssem, rsem, own, fsem, wsem, hsem, esem, a1s, a1r, a2s, a2r, a3s, a3r):
    here = Place()
    z, s, zn, zf, x, y, core = here.z, here.s, here.zn, here.zf, here.x, here.y, here.core
    n_block = w_all.shape[0]
    n_v = n_block // n_stage
    rows = h.shape[1]
    tile = min(WIDE, rows // 2)
    c_g, c_i = narrow(core, x, y), narrow(core, y, x)

    load_e = pltpu.make_async_copy(cot.at[s], e.at[s], esem)
    load_e.start()

    def fetch(b):
        c, slot = n_block - 1 - b, b % 2
        return (
            pltpu.make_async_copy(w_all.at[c], w.at[slot], wsem.at[slot]),
            pltpu.make_async_copy(h_all.at[c], h.at[slot], hsem.at[slot]),
        )

    for copy in fetch(0):
        copy.start()
    enter(here, n_stage)
    load_e.wait()

    def total(phase, slot):
        if phase == 1:
            return x1.at[slot]
        if phase == 2:
            return x1.at[slot, :, :, :, :, 0:WIDE]
        if phase == 3:
            return x1.at[slot, :, :, :, :, 0:LANE]
        if phase == 4:
            return x1.at[slot, :, :, 0, :, 0:LANE]
        return x1.at[slot, :, 0, 0, :, 0:LANE]

    def push(phase, b, moves):
        slot = b % SLOTS
        for src, dst, to in moves:
            remote(src, dst, ssem.at[phase - 1, slot], rsem.at[phase - 1, slot], to).start()

    def taken(phase, b):
        slot = b % SLOTS
        wait_bytes(total(phase, slot), rsem.at[phase - 1, slot])
        wait_bytes(total(phase, slot), ssem.at[phase - 1, slot])

    def when_valid(b, fn):
        @pl.when((b >= 0) & (b < n_block))
        def _():
            fn(b)

    def q1(b):
        push(1, b, ((g.at[b % 2, :, :, :, :, col(HALF - HALF * core, HALF)], x1.at[b % SLOTS], here.to_core),))

    def q2(b):
        taken(1, b)
        q, p = b % SLOTS, b % 2
        for m in range(3):
            for f in range(2):
                for k in range(2):
                    x1[q, m, f, k] += g[p, m, f, k, :, col(HALF * core, HALF)]
        push(2, b, (
            (x1.at[q, 0, :, :, :, col(WIDE - WIDE * x, WIDE)], x2g.at[q], here.to_x),
            (x1.at[q, 1, :, :, :, col(WIDE - WIDE * y, WIDE)], x2i.at[q], here.to_y),
            (x1.at[q, 2, :, 1 - zn], x2o.at[q], here.to_zn),
        ))

    def q3(b):
        taken(2, b)
        q = b % SLOTS
        for f in range(2):
            for k in range(2):
                x2g[q, f, k] += x1[q, 0, f, k, :, col(WIDE * x, WIDE)]
                x2i[q, f, k] += x1[q, 1, f, k, :, col(WIDE * y, WIDE)]
            x2o[q, f] += x1[q, 2, f, zn]
        push(3, b, (
            (x2g.at[q, :, :, :, col(LANE - LANE * y, LANE)], x3g.at[q], here.to_y),
            (x2i.at[q, :, :, :, col(LANE - LANE * x, LANE)], x3i.at[q], here.to_x),
            (x2o.at[q, :, 0:SUB, col(WIDE - WIDE * x, WIDE)], x3a.at[q], here.to_x),
            (x2o.at[q, :, SUB:PIECE, col(WIDE - WIDE * y, WIDE)], x3b.at[q], here.to_y),
        ))

    def q4(b):
        taken(3, b)
        q = b % SLOTS
        for f in range(2):
            for k in range(2):
                x3g[q, f, k] += x2g[q, f, k, :, col(LANE * y, LANE)]
                x3i[q, f, k] += x2i[q, f, k, :, col(LANE * x, LANE)]
            x3a[q, f] += x2o[q, f, 0:SUB, col(WIDE * x, WIDE)]
            x3b[q, f] += x2o[q, f, SUB:PIECE, col(WIDE * y, WIDE)]
        push(4, b, (
            (x3g.at[q, :, 1 - zn], x4g.at[q], here.to_zn),
            (x3i.at[q, :, 1 - zn], x4i.at[q], here.to_zn),
            (x3a.at[q, :, :, col(LANE - LANE * y, LANE)], x4a.at[q], here.to_y),
            (x3b.at[q, :, :, col(LANE - LANE * x, LANE)], x4b.at[q], here.to_x),
        ))

    def q5(b):
        taken(4, b)
        q = b % SLOTS
        for f in range(2):
            x4g[q, f] += x3g[q, f, zn]
            x4i[q, f] += x3i[q, f, zn]
            x4a[q, f] += x3a[q, f, :, col(LANE * y, LANE)]
            x4b[q, f] += x3b[q, f, :, col(LANE * x, LANE)]
        push(5, b, (
            (x4g.at[q, 1 - zf], x5g.at[q], here.to_zf),
            (x4i.at[q, 1 - zf], x5i.at[q], here.to_zf),
            (x4a.at[q, 1 - zf], x5a.at[q], here.to_zf),
            (x4b.at[q, 1 - zf], x5b.at[q], here.to_zf),
        ))

    def q6(b):
        taken(5, b)
        q = b % SLOTS
        c = n_block - 1 - b
        v, p = c // n_stage, c % n_stage
        fg[b] = x5g[q] + x4g[q, zf]
        fi[b] = x5i[q] + x4i[q, zf]
        fa[b] = x5a[q] + x4a[q, zf]
        fb[b] = x5b[q] + x4b[q, zf]
        moves = (
            (fg.at[b], gg.at[v, 0, :, col(c_g, LANE)]),
            (fi.at[b], gi.at[v, 0, :, col(c_i, LANE)]),
            (fa.at[b], go.at[v, 0, pl.ds(pl.multiple_of(PIECE * (2 * core + x), SUB), SUB), col(LANE * y, LANE)]),
            (fb.at[b], go.at[v, 0, pl.ds(pl.multiple_of(PIECE * (2 * core + y) + SUB, SUB), SUB), col(LANE * x, LANE)]),
        )

        @pl.when(p == s)
        def _():
            for src, dst in moves:
                pltpu.make_async_copy(src, dst, own.at[b]).start()

        @pl.when(p != s)
        def _():
            for src, dst in moves:
                remote(src, dst, own.at[b], fsem.at[v], (z, p)).start()

    def one_tile(b, i):
        at = pl.ds(pl.multiple_of(i * tile, tile), tile)
        p = b % 2
        first = i == 0
        x32 = h[p, at, :].astype(F32)
        inv = lax.rsqrt(jnp.mean(x32 * x32, axis=-1, keepdims=True) + NORM_EPS)
        hr = x32 * inv
        n = hr.astype(BF16)
        et = e[s, at, :]
        q = jnp.zeros((tile, WIDE), F32)

        def add(m, k, value):
            for f in range(2):
                for r in range(2):
                    part = value[LANE * f + PIECE * r : LANE * f + PIECE * r + PIECE]
                    old = g[p, m, f, r, :, WIDE * k : WIDE * k + WIDE]
                    g[p, m, f, r, :, WIDE * k : WIDE * k + WIDE] = part + jnp.where(first, 0.0, old)

        for k in range(4):
            wg, wi, wo = square(w, p, 0, k), square(w, p, 1, k), out_square(w, p, k)
            a = mat(n, wg)
            bb = mat(n, wi)
            t = mat_cols(et, wo)
            sg = jax.nn.sigmoid(a)
            act = a * sg
            u = (act * bb).astype(BF16)
            da = (t * bb * sg * (1.0 + a * (1.0 - sg))).astype(BF16)
            db = (t * act).astype(BF16)
            q += mat_cols(da, wg) + mat_cols(db, wi)
            add(0, k, mat_rows(n, da))
            add(1, k, mat_rows(n, db))
            do = mat_rows(u, et)
            for j in range(4):
                old = g[p, 2, k // 2, k % 2, :, WIDE * j : WIDE * j + WIDE]
                g[p, 2, k // 2, k % 2, :, WIDE * j : WIDE * j + WIDE] = do[PIECE * j : PIECE * j + PIECE] + jnp.where(first, 0.0, old)
        grad = et.astype(F32) + inv * (q - hr * jnp.mean(q * hr, axis=-1, keepdims=True))
        e[s, at, :] = grad.astype(BF16)

    per_half = rows // tile // 2

    def half_step(i, carry):
        b = i // 2

        @pl.when(i % 2 == 0)
        def _():
            when_valid(b - 8, q6)
            when_valid(b - 5, q4)
            when_valid(b - 2, q2)

            @pl.when(b < n_block)
            def _():
                for copy in fetch(b):
                    copy.wait()

            @pl.when(b + 1 < n_block)
            def _():
                for copy in fetch(b + 1):
                    copy.start()

        @pl.when(i % 2 == 1)
        def _():
            when_valid(b - 6, q5)
            when_valid(b - 3, q3)

        @pl.when(b < n_block)
        def _():
            def body(j, carry):
                one_tile(b, (i % 2) * per_half + j)
                return carry

            lax.fori_loop(0, per_half, body, 0)

            @pl.when(i % 2 == 1)
            def _():
                q1(b)

        return carry

    lax.fori_loop(0, 2 * n_block, half_step, 0)

    half = rows // 2
    lo, hi = pl.ds(0, half), pl.ds(half, half)
    sx, sy = here.to_x[1], here.to_y[1]
    first = [remote(e.at[s, lo], e.at[s, lo], a1s.at[0], a1r.at[0], here.to_x), remote(e.at[s, hi], e.at[s, hi], a1s.at[1], a1r.at[1], here.to_y)]
    for copy in first:
        copy.start()
    lax.fori_loop(2 * n_block, 2 * n_block + 4, half_step, 0)
    for copy in first:
        copy.wait()
    second = [
        remote(e.at[s, lo], e.at[s, lo], a2s.at[0], a2r.at[0], here.to_y),
        remote(e.at[sx, lo], e.at[sx, lo], a2s.at[1], a2r.at[1], here.to_y),
        remote(e.at[s, hi], e.at[s, hi], a2s.at[2], a2r.at[2], here.to_x),
        remote(e.at[sy, hi], e.at[sy, hi], a2s.at[3], a2r.at[3], here.to_x),
    ]
    for copy in second:
        copy.start()
    lax.fori_loop(2 * n_block + 4, 2 * (n_block + BWD_DRAIN) + 1, half_step, 0)
    for copy in second:
        copy.wait()
    last = []
    for k in range(n_stage // 2):
        q = 2 * k + core
        last.append(remote(e.at[q], ga.at[q], a3s.at[k], a3r.at[k], here.to_core))
        last.append(pltpu.make_async_copy(e.at[q], ga.at[q], a3s.at[n_stage // 2 + k]))
    for copy in last:
        copy.start()

    def finish(b, carry):
        wait_bytes(total(5, 0), own.at[b])
        return carry

    lax.fori_loop(0, n_block, finish, 0)
    for v in range(n_v):
        wait_bytes(g.at[0, :, 0, 0, :, 0 : LANE * (n_stage - 1)], fsem.at[v])
    for copy in last:
        copy.wait()


def solution(mesh):
    n_stage = mesh.shape["stage"]
    act_spec = P(None, "data", None, None)
    w_spec = P(None, "stage", "data", None)
    hbm = pl.BlockSpec(memory_space=pltpu.HBM)
    dma = pltpu.SemaphoreType.DMA

    def body(act_in, cot_out, w_gate, w_in, w_out):
        n_micro, n_seq, n_tok, width = act_in.shape
        n_v, _, _, ffn = w_gate.shape
        n_block = n_v * n_stage
        rows = n_micro // n_stage * n_seq * n_tok
        act = act_in.reshape(n_stage, rows, width)
        cot = cot_out.reshape(n_stage, rows, width)
        block = (3, 2, 2, PIECE, ffn)
        flops = 2 * rows * width * ffn * n_block

        def f32(*shape):
            return pltpu.VMEM(shape, F32)

        w_all, h_all = pl.pallas_call(
            functools.partial(fwd_kernel, n_stage),
            name="forward",
            out_shape=(jax.ShapeDtypeStruct((n_block, *block), BF16), jax.ShapeDtypeStruct((n_block, rows, width), BF16)),
            in_specs=[hbm] * 4,
            out_specs=[hbm] * 2,
            scratch_shapes=[
                pltpu.VMEM((n_block, *block), BF16),
                pltpu.VMEM((n_block, rows, width), BF16),
                dma((n_v,)),
                dma((n_block,)),
                dma((5, SLOTS)),
                dma((5, SLOTS)),
                dma,
                dma((n_block,)),
                dma((n_block,)),
            ],
            compiler_params=pltpu.CompilerParams(collective_id=0, has_side_effects=True, vmem_limit_bytes=63 * 2**20),
            cost_estimate=pl.CostEstimate(flops=3 * flops, bytes_accessed=2**26, transcendentals=0),
        )(act, w_gate, w_in, w_out)
        n = SLOTS
        gg, gi, go, ga = pl.pallas_call(
            functools.partial(bwd_kernel, n_stage),
            name="backward",
            out_shape=(
                jax.ShapeDtypeStruct(w_gate.shape, F32),
                jax.ShapeDtypeStruct(w_in.shape, F32),
                jax.ShapeDtypeStruct(w_out.shape, F32),
                jax.ShapeDtypeStruct((n_stage, rows, width), BF16),
            ),
            in_specs=[hbm] * 3,
            out_specs=[hbm] * 4,
            scratch_shapes=[
                pltpu.VMEM((2, *block), BF16),
                pltpu.VMEM((2, rows, width), BF16),
                pltpu.VMEM((n_stage, rows, width), BF16),
                f32(2, *block),
                f32(n, 3, 2, 2, PIECE, HALF),
                f32(n, 2, 2, PIECE, WIDE),
                f32(n, 2, 2, PIECE, WIDE),
                f32(n, 2, PIECE, HALF),
                f32(n, 2, 2, PIECE, LANE),
                f32(n, 2, 2, PIECE, LANE),
                f32(n, 2, SUB, WIDE),
                f32(n, 2, SUB, WIDE),
                f32(n, 2, PIECE, LANE),
                f32(n, 2, PIECE, LANE),
                f32(n, 2, SUB, LANE),
                f32(n, 2, SUB, LANE),
                f32(n, PIECE, LANE),
                f32(n, PIECE, LANE),
                f32(n, SUB, LANE),
                f32(n, SUB, LANE),
                f32(n_block, PIECE, LANE),
                f32(n_block, PIECE, LANE),
                f32(n_block, SUB, LANE),
                f32(n_block, SUB, LANE),
                dma((5, SLOTS)),
                dma((5, SLOTS)),
                dma((n_block,)),
                dma((n_v,)),
                dma((2,)),
                dma((2,)),
                dma,
                dma((2,)),
                dma((2,)),
                dma((4,)),
                dma((4,)),
                dma((n_stage,)),
                dma((n_stage // 2,)),
            ],
            compiler_params=pltpu.CompilerParams(collective_id=1, has_side_effects=True, vmem_limit_bytes=63 * 2**20),
            cost_estimate=pl.CostEstimate(flops=8 * flops, bytes_accessed=2**26, transcendentals=0),
        )(cot, w_all, h_all)
        return ga.reshape(act_in.shape), gg, gi, go

    return jax.shard_map(body, mesh=mesh, in_specs=(act_spec, act_spec, w_spec, w_spec, w_spec), out_specs=(act_spec, w_spec, w_spec, w_spec), check_vma=False)
```

```python
import functools

import jax
import jax.numpy as jnp
from jax import lax
from jax.experimental import pallas as pl
from jax.experimental.pallas import tpu as pltpu
from jax.sharding import PartitionSpec as P

NORM_EPS = 1e-6
MESH = pl.DeviceIdType.MESH
SLOTS = 8
FWD_LEAD = 7
TICKS = 6
Q_AT = (0, 6, 8, 18, 28, 39, 54)
RELAY_AT = 22
LANE, WIDE, HALF = 128, 256, 512
PIECE, SUB = 64, 32
LO, HI = slice(0, SUB), slice(SUB, PIECE)
F32 = jnp.float32
BF16 = jnp.bfloat16


class Place:
    def __init__(self):
        self.z, self.s = lax.axis_index("data"), lax.axis_index("stage")
        self.core, self.x, self.y = self.s % 2, (self.s // 2) % 2, self.s // 4
        self.zn, self.zf = self.z % 2, self.z // 2
        self.to_x = (self.z, self.s + 2 - 4 * self.x)
        self.to_y = (self.z, self.s + 4 - 8 * self.y)
        self.to_core = (self.z, self.s + 1 - 2 * self.core)
        self.to_zn = (self.z + 1 - 2 * self.zn, self.s)
        self.to_zf = (self.z + 2 - 4 * self.zf, self.s)


def col(start, size):
    return pl.ds(pl.multiple_of(start, LANE), size)


def narrow(core, hi, lo):
    return HALF * core + WIDE * hi + LANE * lo


def remote(src, dst, ssem, rsem, to):
    return pltpu.make_async_remote_copy(src_ref=src, dst_ref=dst, send_sem=ssem, recv_sem=rsem, device_id=to, device_id_type=MESH)


def wait_bytes(ref, sem):
    pltpu.make_async_copy(ref, ref, sem).wait()


def enter(here, n_stage):
    barrier = pltpu.get_barrier_semaphore()
    peers = [(here.z, (here.s + k) % n_stage) for k in range(1, n_stage)] + [here.to_zn, here.to_zf]
    for peer in peers:
        pl.semaphore_signal(barrier, inc=1, device_id=peer, device_id_type=MESH)
    pl.semaphore_wait(barrier, len(peers))


def mat_rows(left, right):
    return lax.dot_general(left, right, (((0,), (0,)), ((), ())), preferred_element_type=F32)


def mat_cols(left, right):
    return lax.dot_general(left, right, (((1,), (1,)), ((), ())), preferred_element_type=F32)


def mat(left, right):
    return jnp.dot(left, right, preferred_element_type=F32)


def square(w_ref, at, m, k):
    return w_ref[at, m, :, :, :, WIDE * k : WIDE * k + WIDE].reshape(WIDE, WIDE)


def out_square(w_ref, at, k):
    return jnp.concatenate([w_ref[at, 2, k // 2, k % 2, :, WIDE * j : WIDE * j + WIDE] for j in range(4)], axis=0)


def fwd_kernel(n_stage, act, wg, wi, wo, w_all, h_all, w, h, s0, r0, ssem, rsem, lsem, hsem, wsem):
    here = Place()
    z, s, zn, zf = here.z, here.s, here.zn, here.zf
    n_block = w.shape[0]
    n_v = n_block // n_stage
    rows = h.shape[1]
    tile = min(WIDE, rows // 2)
    c_g, c_i = narrow(here.core, here.x, here.y), narrow(here.core, here.y, here.x)
    c_x, c_y, c_c = narrow(here.core, here.x, 0), narrow(here.core, here.y, 0), narrow(here.core, 0, 0)

    enter(here, n_stage)
    load = pltpu.make_async_copy(act.at[s], h.at[0], lsem)
    load.start()

    def scatter(v, k):
        q = (s + k) % n_stage
        core, x, y = q % 2, (q // 2) % 2, q // 4
        d_g, d_i = narrow(core, x, y), narrow(core, y, x)
        c = v * n_stage + s
        moves = (
            (wg.at[v, 0, :, col(d_g, LANE)], w.at[c, 0, zf, zn, :, col(d_g, LANE)]),
            (wi.at[v, 0, :, col(d_i, LANE)], w.at[c, 1, zf, zn, :, col(d_i, LANE)]),
            (wo.at[v, 0, pl.ds(pl.multiple_of(PIECE * (2 * core + x), SUB), SUB), col(LANE * y, LANE)], w.at[c, 2, zf, zn, 0:SUB, col(d_g, LANE)]),
            (wo.at[v, 0, pl.ds(pl.multiple_of(PIECE * (2 * core + y) + SUB, SUB), SUB), col(LANE * x, LANE)], w.at[c, 2, zf, zn, SUB:PIECE, col(d_i, LANE)]),
        )
        for src, dst in moves:
            if k == 0:
                pltpu.make_async_copy(src, dst, r0.at[c]).start()
            else:
                remote(src, dst, s0.at[v], r0.at[c], (z, q)).start()

    for v in range(n_v):
        for k in range(n_stage):
            scatter(v, k)

    def parts(phase, c):
        if phase == 1:
            return (
                (w.at[c, 0, zf, zn, :, col(c_g, LANE)], here.to_zf),
                (w.at[c, 1, zf, zn, :, col(c_i, LANE)], here.to_zf),
                (w.at[c, 2, zf, zn, 0:SUB, col(c_g, LANE)], here.to_zf),
                (w.at[c, 2, zf, zn, SUB:PIECE, col(c_i, LANE)], here.to_zf),
            )
        if phase == 2:
            return (
                (w.at[c, 0, :, zn, :, col(c_g, LANE)], here.to_zn),
                (w.at[c, 1, :, zn, :, col(c_i, LANE)], here.to_zn),
                (w.at[c, 2, :, zn, 0:SUB, col(c_g, LANE)], here.to_y),
                (w.at[c, 2, :, zn, SUB:PIECE, col(c_i, LANE)], here.to_x),
            )
        if phase == 3:
            return (
                (w.at[c, 0, :, :, :, col(c_g, LANE)], here.to_y),
                (w.at[c, 1, :, :, :, col(c_i, LANE)], here.to_x),
                (w.at[c, 2, :, zn, 0:SUB, col(c_x, WIDE)], here.to_x),
                (w.at[c, 2, :, zn, SUB:PIECE, col(c_y, WIDE)], here.to_y),
            )
        if phase == 4:
            return (
                (w.at[c, 0, :, :, :, col(c_x, WIDE)], here.to_x),
                (w.at[c, 1, :, :, :, col(c_y, WIDE)], here.to_y),
                (w.at[c, 2, :, zn, :, col(c_c, HALF)], here.to_zn),
            )
        return ((w.at[c, :, :, :, :, col(c_c, HALF)], here.to_core),)

    def total(phase, c):
        if phase == 1:
            return w.at[c, :, 0, 0, :, 0:LANE]
        if phase == 2:
            return w.at[c, :, :, 0, :, 0:LANE]
        return w.at[c, :, :, :, :, 0 : {3: LANE, 4: WIDE, 5: HALF}[phase]]

    def arrived(phase, c):
        if phase == 0:
            wait_bytes(total(1, c), r0.at[c])
        else:
            slot = c % SLOTS
            wait_bytes(total(phase, c), rsem.at[phase - 1, slot])
            wait_bytes(total(phase, c), ssem.at[phase - 1, slot])

    def advance(phase, c):
        @pl.when((c >= 0) & (c < n_block))
        def _():
            arrived(phase - 1, c)
            slot = c % SLOTS
            for ref, to in parts(phase, c):
                remote(ref, ref, ssem.at[phase - 1, slot], rsem.at[phase - 1, slot], to).start()

    def one_tile(c, i):
        at = pl.ds(pl.multiple_of(i * tile, tile), tile)
        x32 = h[c, at, :].astype(F32)
        inv = lax.rsqrt(jnp.mean(x32 * x32, axis=-1, keepdims=True) + NORM_EPS)
        n = (x32 * inv).astype(BF16)
        acc = x32
        for k in range(4):
            a = mat(n, square(w, c, 0, k))
            b = mat(n, square(w, c, 1, k))
            u = (a * jax.nn.sigmoid(a) * b).astype(BF16)
            acc += mat(u, out_square(w, c, k))
        h[c + 1, at, :] = acc.astype(BF16)

    per_half = rows // tile // 2

    def half_step(i, carry):
        c = i // 2 - FWD_LEAD
        second = i % 2 == 1

        @pl.when(i % 2 == 0)
        def _():
            advance(4, c + 2)
            advance(2, c + 5)

            @pl.when(c == 0)
            def _():
                load.wait()

            @pl.when(c >= 0)
            def _():
                arrived(5, c)

        @pl.when(second)
        def _():
            advance(5, c + 1)
            advance(3, c + 4)
            advance(1, c + 7)

            @pl.when(c >= 0)
            def _():
                pltpu.make_async_copy(w.at[c], w_all.at[c], wsem.at[c]).start()
                pltpu.make_async_copy(h.at[c], h_all.at[c], hsem.at[c]).start()

        @pl.when((c >= 0) & (c < n_block - 1))
        def _():
            def body(j, carry):
                one_tile(c, (i % 2) * per_half + j)
                return carry

            lax.fori_loop(0, per_half, body, 0)

        return carry

    lax.fori_loop(0, 2 * (n_block + FWD_LEAD), half_step, 0)
    for v in range(n_v):
        wait_bytes(w.at[0, :, 0, 0, :, 0 : LANE * (n_stage - 1)], s0.at[v])

    def drain(c, carry):
        pltpu.make_async_copy(w.at[c], w_all.at[c], wsem.at[c]).wait()
        pltpu.make_async_copy(h.at[c], h_all.at[c], hsem.at[c]).wait()
        return carry

    lax.fori_loop(0, n_block, drain, 0)


def bwd_kernel(n_stage, cot, w_all, h_all, gg, gi, go, ga, w, h, e, g, x1, x2g, x2i, x2o, x3gl, x3il, x3gh, x3ih, x3a, x3b, x4g, x4i, x4a, x4b, x5g, x5i, x5a, x5b, fg, fi, fa, fb, ssem, rsem, own, fsem, wsem, hsem, esem, as_, ar, cs, cr, cl):
    here = Place()
    z, s, zn, zf, x, y, core = here.z, here.s, here.zn, here.zf, here.x, here.y, here.core
    n_block = w_all.shape[0]
    n_v = n_block // n_stage
    rows = h.shape[1]
    tile = rows // TICKS
    c_g, c_i = narrow(core, x, y), narrow(core, y, x)

    load_e = pltpu.make_async_copy(cot.at[s], e.at[s], esem)
    load_e.start()

    def fetch(b):
        c, slot = n_block - 1 - b, b % 2
        return (
            pltpu.make_async_copy(w_all.at[c], w.at[slot], wsem.at[slot]),
            pltpu.make_async_copy(h_all.at[c], h.at[slot], hsem.at[slot]),
        )

    for copy in fetch(0):
        copy.start()
    enter(here, n_stage)
    load_e.wait()

    def total(phase, slot):
        if phase == 1:
            return x1.at[slot]
        if phase == 2:
            return x1.at[slot, :, :, :, :, 0:WIDE]
        if phase == 3:
            return x1.at[slot, :, :, :, :, 0:LANE]
        if phase == 4:
            return x1.at[slot, :, :, 0, :, 0:LANE]
        return x1.at[slot, :, 0, 0, :, 0:LANE]

    def push(phase, b, moves):
        slot = b % SLOTS
        for src, dst, to in moves:
            remote(src, dst, ssem.at[phase - 1, slot], rsem.at[phase - 1, slot], to).start()

    def taken(phase, b):
        slot = b % SLOTS
        wait_bytes(total(phase, slot), rsem.at[phase - 1, slot])
        wait_bytes(total(phase, slot), ssem.at[phase - 1, slot])

    def when_valid(b, fn):
        @pl.when((b >= 0) & (b < n_block))
        def _():
            fn(b)

    def q1(b):
        push(1, b, ((g.at[b % 2, :, :, :, :, col(HALF - HALF * core, HALF)], x1.at[b % SLOTS], here.to_core),))

    def q2(b):
        taken(1, b)
        q, p = b % SLOTS, b % 2
        for m in range(3):
            for f in range(2):
                for k in range(2):
                    x1[q, m, f, k] += g[p, m, f, k, :, col(HALF * core, HALF)]
        push(2, b, (
            (x1.at[q, 0, :, :, :, col(WIDE - WIDE * x, WIDE)], x2g.at[q], here.to_x),
            (x1.at[q, 1, :, :, :, col(WIDE - WIDE * y, WIDE)], x2i.at[q], here.to_y),
            (x1.at[q, 2, :, 1 - zn], x2o.at[q], here.to_zn),
        ))

    def q3(b):
        taken(2, b)
        q = b % SLOTS
        for f in range(2):
            for k in range(2):
                x2g[q, f, k] += x1[q, 0, f, k, :, col(WIDE * x, WIDE)]
                x2i[q, f, k] += x1[q, 1, f, k, :, col(WIDE * y, WIDE)]
            x2o[q, f] += x1[q, 2, f, zn]
        push(3, b, (
            (x2g.at[q, :, :, LO, col(LANE - LANE * y, LANE)], x3gl.at[q], here.to_y),
            (x2i.at[q, :, :, LO, col(LANE - LANE * x, LANE)], x3il.at[q], here.to_x),
            (x2g.at[q, :, 1 - zn, HI], x3gh.at[q], here.to_zn),
            (x2i.at[q, :, 1 - zn, HI], x3ih.at[q], here.to_zn),
            (x2o.at[q, :, LO, col(WIDE - WIDE * x, WIDE)], x3a.at[q], here.to_x),
            (x2o.at[q, :, HI, col(WIDE - WIDE * y, WIDE)], x3b.at[q], here.to_y),
        ))

    def q4(b):
        taken(3, b)
        q = b % SLOTS
        for f in range(2):
            for k in range(2):
                x3gl[q, f, k] += x2g[q, f, k, LO, col(LANE * y, LANE)]
                x3il[q, f, k] += x2i[q, f, k, LO, col(LANE * x, LANE)]
            x3gh[q, f] += x2g[q, f, zn, HI]
            x3ih[q, f] += x2i[q, f, zn, HI]
            x3a[q, f] += x2o[q, f, LO, col(WIDE * x, WIDE)]
            x3b[q, f] += x2o[q, f, HI, col(WIDE * y, WIDE)]
        push(4, b, (
            (x3gl.at[q, :, 1 - zn], x4g.at[q, :, LO], here.to_zn),
            (x3il.at[q, :, 1 - zn], x4i.at[q, :, LO], here.to_zn),
            (x3gh.at[q, :, :, col(LANE - LANE * y, LANE)], x4g.at[q, :, HI], here.to_y),
            (x3ih.at[q, :, :, col(LANE - LANE * x, LANE)], x4i.at[q, :, HI], here.to_x),
            (x3a.at[q, :, :, col(LANE - LANE * y, LANE)], x4a.at[q], here.to_y),
            (x3b.at[q, :, :, col(LANE - LANE * x, LANE)], x4b.at[q], here.to_x),
        ))

    def q5(b):
        taken(4, b)
        q = b % SLOTS
        for f in range(2):
            x4g[q, f, LO] += x3gl[q, f, zn]
            x4i[q, f, LO] += x3il[q, f, zn]
            x4g[q, f, HI] += x3gh[q, f, :, col(LANE * y, LANE)]
            x4i[q, f, HI] += x3ih[q, f, :, col(LANE * x, LANE)]
            x4a[q, f] += x3a[q, f, :, col(LANE * y, LANE)]
            x4b[q, f] += x3b[q, f, :, col(LANE * x, LANE)]
        push(5, b, (
            (x4g.at[q, 1 - zf], x5g.at[q], here.to_zf),
            (x4i.at[q, 1 - zf], x5i.at[q], here.to_zf),
            (x4a.at[q, 1 - zf], x5a.at[q], here.to_zf),
            (x4b.at[q, 1 - zf], x5b.at[q], here.to_zf),
        ))

    def q6(b):
        taken(5, b)
        q = b % SLOTS
        c = n_block - 1 - b
        v, p = c // n_stage, c % n_stage
        fg[b] = x5g[q] + x4g[q, zf]
        fi[b] = x5i[q] + x4i[q, zf]
        fa[b] = x5a[q] + x4a[q, zf]
        fb[b] = x5b[q] + x4b[q, zf]
        moves = (
            (fg.at[b], gg.at[v, 0, :, col(c_g, LANE)]),
            (fi.at[b], gi.at[v, 0, :, col(c_i, LANE)]),
            (fa.at[b], go.at[v, 0, pl.ds(pl.multiple_of(PIECE * (2 * core + x), SUB), SUB), col(LANE * y, LANE)]),
            (fb.at[b], go.at[v, 0, pl.ds(pl.multiple_of(PIECE * (2 * core + y) + SUB, SUB), SUB), col(LANE * x, LANE)]),
        )

        @pl.when(p == s)
        def _():
            for src, dst in moves:
                pltpu.make_async_copy(src, dst, own.at[b]).start()

        @pl.when(p != s)
        def _():
            for src, dst in moves:
                remote(src, dst, own.at[b], fsem.at[v], (z, p)).start()

    def one_tile(b, i):
        at = pl.ds(pl.multiple_of(i * tile, tile), tile)
        p = b % 2
        first = i == 0
        x32 = h[p, at, :].astype(F32)
        inv = lax.rsqrt(jnp.mean(x32 * x32, axis=-1, keepdims=True) + NORM_EPS)
        hr = x32 * inv
        n = hr.astype(BF16)
        et = e[s, at, :]
        q = jnp.zeros((tile, WIDE), F32)

        def add(m, k, value):
            for f in range(2):
                for r in range(2):
                    part = value[LANE * f + PIECE * r : LANE * f + PIECE * r + PIECE]
                    old = g[p, m, f, r, :, WIDE * k : WIDE * k + WIDE]
                    g[p, m, f, r, :, WIDE * k : WIDE * k + WIDE] = part + jnp.where(first, 0.0, old)

        for k in range(4):
            wg, wi, wo = square(w, p, 0, k), square(w, p, 1, k), out_square(w, p, k)
            a = mat(n, wg)
            bb = mat(n, wi)
            t = mat_cols(et, wo)
            sg = jax.nn.sigmoid(a)
            act = a * sg
            u = (act * bb).astype(BF16)
            da = (t * bb * sg * (1.0 + a * (1.0 - sg))).astype(BF16)
            db = (t * act).astype(BF16)
            q += mat_cols(da, wg) + mat_cols(db, wi)
            add(0, k, mat_rows(n, da))
            add(1, k, mat_rows(n, db))
            do = mat_rows(u, et)
            for j in range(4):
                old = g[p, 2, k // 2, k % 2, :, WIDE * j : WIDE * j + WIDE]
                g[p, 2, k // 2, k % 2, :, WIDE * j : WIDE * j + WIDE] = do[PIECE * j : PIECE * j + PIECE] + jnp.where(first, 0.0, old)
        grad = et.astype(F32) + inv * (q - hr * jnp.mean(q * hr, axis=-1, keepdims=True))
        e[s, at, :] = grad.astype(BF16)

    def step(i, carry):
        for k, fn in ((6, q6), (5, q5), (4, q4), (3, q3), (2, q2), (1, q1)):
            since = i - Q_AT[k]

            @pl.when((since >= 0) & (since < TICKS * n_block) & ((since + TICKS * n_block) % TICKS == 0))
            def _(fn=fn, since=since):
                fn(since // TICKS)

        @pl.when(i < TICKS * n_block)
        def _():
            b = i // TICKS

            @pl.when(i % TICKS == 0)
            def _():
                for copy in fetch(b):
                    copy.wait()

                @pl.when(b + 1 < n_block)
                def _():
                    for copy in fetch(b + 1):
                        copy.start()

            one_tile(b, i % TICKS)

        return carry

    half = rows // 2
    lo, hi = pl.ds(0, half), pl.ds(half, half)
    sx, sy = here.to_x[1], here.to_y[1]
    sd = 2 * ((sx // 2 + sy // 2 - s // 2) % (n_stage // 2)) + core

    def share(k, slot, part, to):
        return remote(e.at[slot, part], e.at[slot, part], as_.at[k], ar.at[k], to)

    first = (share(0, s, lo, here.to_x), share(1, s, lo, here.to_y), share(2, s, hi, here.to_y), share(3, s, hi, here.to_x))
    relay = (share(4, sx, lo, here.to_y), share(5, sy, hi, here.to_x))

    def hand(k, slot):
        return (
            remote(e.at[slot], ga.at[slot], cs.at[k], cr.at[k], here.to_core),
            pltpu.make_async_copy(e.at[slot], ga.at[slot], cl.at[k]),
        )

    hands = [hand(k, slot) for k, slot in enumerate((s, sx, sy, sd))]
    last = TICKS * n_block
    lax.fori_loop(0, last - TICKS // 2, step, 0)
    for copy in first[:2]:
        copy.start()
    lax.fori_loop(last - TICKS // 2, last, step, 0)
    for copy in first[2:]:
        copy.start()
    lax.fori_loop(last, last + RELAY_AT, step, 0)
    first[0].wait_recv()
    relay[0].start()
    first[2].wait_recv()
    relay[1].start()
    for copy in hands[0]:
        copy.start()
    lax.fori_loop(last + RELAY_AT, last + Q_AT[6], step, 0)
    first[3].wait_recv()
    for copy in hands[1]:
        copy.start()
    first[1].wait_recv()
    for copy in hands[2]:
        copy.start()
    for copy in relay:
        copy.wait_recv()
    for copy in hands[3]:
        copy.start()
    for copy in first + relay:
        copy.wait_send()

    def finish(b, carry):
        wait_bytes(total(5, 0), own.at[b])
        return carry

    lax.fori_loop(0, n_block, finish, 0)
    for v in range(n_v):
        wait_bytes(g.at[0, :, 0, 0, :, 0 : LANE * (n_stage - 1)], fsem.at[v])
    for pair in hands:
        for copy in pair:
            copy.wait()


def settle_kernel(*refs):
    n = (len(refs) - 2) // 3
    srcs, dsts, bufs, (rsem, wsem) = refs[:n], refs[n : 2 * n], refs[2 * n : 3 * n], refs[3 * n :]
    moves = []
    for a in range(n):
        for i in range(srcs[a].shape[0]):
            k = len(moves)
            moves.append((
                pltpu.make_async_copy(srcs[a].at[i], bufs[a].at[i], rsem.at[k]),
                pltpu.make_async_copy(bufs[a].at[i], dsts[a].at[i], wsem.at[k]),
            ))
    for read, _ in moves:
        read.start()
    for read, write in moves:
        read.wait()
        write.start()
    for _, write in moves:
        write.wait()


def solution(mesh):
    n_stage = mesh.shape["stage"]
    act_spec = P(None, "data", None, None)
    w_spec = P(None, "stage", "data", None)
    hbm = pl.BlockSpec(memory_space=pltpu.HBM)
    dma = pltpu.SemaphoreType.DMA

    def body(act_in, cot_out, w_gate, w_in, w_out):
        n_micro, n_seq, n_tok, width = act_in.shape
        n_v, _, _, ffn = w_gate.shape
        n_block = n_v * n_stage
        rows = n_micro // n_stage * n_seq * n_tok
        act = act_in.reshape(n_stage, rows, width)
        cot = cot_out.reshape(n_stage, rows, width)
        block = (3, 2, 2, PIECE, ffn)
        flops = 2 * rows * width * ffn * n_block

        def f32(*shape):
            return pltpu.VMEM(shape, F32)

        w_all, h_all = pl.pallas_call(
            functools.partial(fwd_kernel, n_stage),
            name="forward",
            out_shape=(jax.ShapeDtypeStruct((n_block, *block), BF16), jax.ShapeDtypeStruct((n_block, rows, width), BF16)),
            in_specs=[hbm] * 4,
            out_specs=[hbm] * 2,
            scratch_shapes=[
                pltpu.VMEM((n_block, *block), BF16),
                pltpu.VMEM((n_block, rows, width), BF16),
                dma((n_v,)),
                dma((n_block,)),
                dma((5, SLOTS)),
                dma((5, SLOTS)),
                dma,
                dma((n_block,)),
                dma((n_block,)),
            ],
            compiler_params=pltpu.CompilerParams(collective_id=0, has_side_effects=True, vmem_limit_bytes=63 * 2**20),
            cost_estimate=pl.CostEstimate(flops=3 * flops, bytes_accessed=2**26, transcendentals=0),
        )(act, w_gate, w_in, w_out)
        n = SLOTS
        gg, gi, go, ga = pl.pallas_call(
            functools.partial(bwd_kernel, n_stage),
            name="backward",
            out_shape=(
                jax.ShapeDtypeStruct(w_gate.shape, F32),
                jax.ShapeDtypeStruct(w_in.shape, F32),
                jax.ShapeDtypeStruct(w_out.shape, F32),
                jax.ShapeDtypeStruct((n_stage, rows, width), BF16),
            ),
            in_specs=[hbm] * 3,
            out_specs=[hbm] * 4,
            scratch_shapes=[
                pltpu.VMEM((2, *block), BF16),
                pltpu.VMEM((2, rows, width), BF16),
                pltpu.VMEM((n_stage, rows, width), BF16),
                f32(2, *block),
                f32(n, 3, 2, 2, PIECE, HALF),
                f32(n, 2, 2, PIECE, WIDE),
                f32(n, 2, 2, PIECE, WIDE),
                f32(n, 2, PIECE, HALF),
                f32(n, 2, 2, SUB, LANE),
                f32(n, 2, 2, SUB, LANE),
                f32(n, 2, SUB, WIDE),
                f32(n, 2, SUB, WIDE),
                f32(n, 2, SUB, WIDE),
                f32(n, 2, SUB, WIDE),
                f32(n, 2, PIECE, LANE),
                f32(n, 2, PIECE, LANE),
                f32(n, 2, SUB, LANE),
                f32(n, 2, SUB, LANE),
                f32(n, PIECE, LANE),
                f32(n, PIECE, LANE),
                f32(n, SUB, LANE),
                f32(n, SUB, LANE),
                f32(n_block, PIECE, LANE),
                f32(n_block, PIECE, LANE),
                f32(n_block, SUB, LANE),
                f32(n_block, SUB, LANE),
                dma((5, SLOTS)),
                dma((5, SLOTS)),
                dma((n_block,)),
                dma((n_v,)),
                dma((2,)),
                dma((2,)),
                dma,
                dma((TICKS,)),
                dma((TICKS,)),
                dma((4,)),
                dma((4,)),
                dma((4,)),
            ],
            compiler_params=pltpu.CompilerParams(collective_id=1, has_side_effects=True, vmem_limit_bytes=63 * 2**20),
            cost_estimate=pl.CostEstimate(flops=8 * flops, bytes_accessed=2**26, transcendentals=0),
        )(cot, w_all, h_all)
        done = (ga, gg, gi, go)
        moved = sum(a.shape[0] for a in done)
        ga, gg, gi, go = pl.pallas_call(
            settle_kernel,
            name="settle",
            out_shape=[jax.ShapeDtypeStruct(a.shape, a.dtype) for a in done],
            in_specs=[hbm] * 4,
            out_specs=[hbm] * 4,
            scratch_shapes=[pltpu.VMEM(a.shape, a.dtype) for a in done] + [dma((moved,)), dma((moved,))],
        )(*done)
        return ga.reshape(act_in.shape), gg, gi, go

    return jax.shard_map(body, mesh=mesh, in_specs=(act_spec, act_spec, w_spec, w_spec, w_spec), out_specs=(act_spec, w_spec, w_spec, w_spec), check_vma=False)
```

```python
import functools

import jax
import jax.numpy as jnp
from jax import lax
from jax.experimental import pallas as pl
from jax.experimental.pallas import tpu as pltpu
from jax.sharding import PartitionSpec as P

NORM_EPS = 1e-6
MESH = pl.DeviceIdType.MESH
SLOTS = 10
TICKS = 3
P_AHEAD = (0, 19, 14, 10, 5, 2)
Q_AT = (0, 3, 5, 10, 19, 27, 37)
RELAY_AT = 20
LANE, WIDE, HALF = 128, 256, 512
PIECE, SUB = 64, 32
LO, HI = slice(0, SUB), slice(SUB, PIECE)
F32 = jnp.float32
BF16 = jnp.bfloat16


class Place:
    def __init__(self):
        self.z, self.s = lax.axis_index("data"), lax.axis_index("stage")
        self.core, self.x, self.y = self.s % 2, (self.s // 2) % 2, self.s // 4
        self.zn, self.zf = self.z % 2, self.z // 2
        self.to_x = (self.z, self.s + 2 - 4 * self.x)
        self.to_y = (self.z, self.s + 4 - 8 * self.y)
        self.to_core = (self.z, self.s + 1 - 2 * self.core)
        self.to_zn = (self.z + 1 - 2 * self.zn, self.s)
        self.to_zf = (self.z + 2 - 4 * self.zf, self.s)


def col(start, size):
    return pl.ds(pl.multiple_of(start, LANE), size)


def narrow(core, hi, lo):
    return HALF * core + WIDE * hi + LANE * lo


def remote(src, dst, ssem, rsem, to):
    return pltpu.make_async_remote_copy(src_ref=src, dst_ref=dst, send_sem=ssem, recv_sem=rsem, device_id=to, device_id_type=MESH)


def wait_bytes(ref, sem):
    pltpu.make_async_copy(ref, ref, sem).wait()


def enter(here, n_stage):
    barrier = pltpu.get_barrier_semaphore()
    peers = [(here.z, (here.s + k) % n_stage) for k in range(1, n_stage)] + [here.to_zn, here.to_zf]
    for peer in peers:
        pl.semaphore_signal(barrier, inc=1, device_id=peer, device_id_type=MESH)
    pl.semaphore_wait(barrier, len(peers))


def mat_rows(left, right):
    return lax.dot_general(left, right, (((0,), (0,)), ((), ())), preferred_element_type=F32)


def mat_cols(left, right):
    return lax.dot_general(left, right, (((1,), (1,)), ((), ())), preferred_element_type=F32)


def mat(left, right):
    return jnp.dot(left, right, preferred_element_type=F32)


def square(w_ref, at, m, k):
    return w_ref[at, m, :, :, :, WIDE * k : WIDE * k + WIDE].reshape(WIDE, WIDE)


def out_square(w_ref, at, k):
    return jnp.concatenate([w_ref[at, 2, k // 2, k % 2, :, WIDE * j : WIDE * j + WIDE] for j in range(4)], axis=0)


def fwd_kernel(n_stage, act, wg, wi, wo, w_all, h_all, w, h, s0, r0, ssem, rsem, lsem, hsem, wsem):
    here = Place()
    z, s, zn, zf = here.z, here.s, here.zn, here.zf
    n_block = w.shape[0]
    n_v = n_block // n_stage
    rows = h.shape[1]
    tile = rows // TICKS
    c_g, c_i = narrow(here.core, here.x, here.y), narrow(here.core, here.y, here.x)
    c_x, c_y, c_c = narrow(here.core, here.x, 0), narrow(here.core, here.y, 0), narrow(here.core, 0, 0)

    enter(here, n_stage)
    load = pltpu.make_async_copy(act.at[s], h.at[0], lsem)
    load.start()

    def scatter(v, k):
        q = (s + k) % n_stage
        core, x, y = q % 2, (q // 2) % 2, q // 4
        d_g, d_i = narrow(core, x, y), narrow(core, y, x)
        c = v * n_stage + s
        moves = (
            (wg.at[v, 0, :, col(d_g, LANE)], w.at[c, 0, zf, zn, :, col(d_g, LANE)]),
            (wi.at[v, 0, :, col(d_i, LANE)], w.at[c, 1, zf, zn, :, col(d_i, LANE)]),
            (wo.at[v, 0, pl.ds(pl.multiple_of(PIECE * (2 * core + x), SUB), SUB), col(LANE * y, LANE)], w.at[c, 2, zf, zn, 0:SUB, col(d_g, LANE)]),
            (wo.at[v, 0, pl.ds(pl.multiple_of(PIECE * (2 * core + y) + SUB, SUB), SUB), col(LANE * x, LANE)], w.at[c, 2, zf, zn, SUB:PIECE, col(d_i, LANE)]),
        )
        for src, dst in moves:
            if k == 0:
                pltpu.make_async_copy(src, dst, r0.at[c]).start()
            else:
                remote(src, dst, s0.at[v], r0.at[c], (z, q)).start()

    for v in range(n_v):
        for k in range(n_stage):
            scatter(v, k)

    def parts(phase, c):
        if phase == 1:
            return (
                (w.at[c, 0, zf, zn, :, col(c_g, LANE)], here.to_zf),
                (w.at[c, 1, zf, zn, :, col(c_i, LANE)], here.to_zf),
                (w.at[c, 2, zf, zn, 0:SUB, col(c_g, LANE)], here.to_zf),
                (w.at[c, 2, zf, zn, SUB:PIECE, col(c_i, LANE)], here.to_zf),
            )
        if phase == 2:
            return (
                (w.at[c, 0, :, zn, :, col(c_g, LANE)], here.to_zn),
                (w.at[c, 1, :, zn, :, col(c_i, LANE)], here.to_zn),
                (w.at[c, 2, :, zn, 0:SUB, col(c_g, LANE)], here.to_y),
                (w.at[c, 2, :, zn, SUB:PIECE, col(c_i, LANE)], here.to_x),
            )
        if phase == 3:
            return (
                (w.at[c, 0, :, :, :, col(c_g, LANE)], here.to_y),
                (w.at[c, 1, :, :, :, col(c_i, LANE)], here.to_x),
                (w.at[c, 2, :, zn, 0:SUB, col(c_x, WIDE)], here.to_x),
                (w.at[c, 2, :, zn, SUB:PIECE, col(c_y, WIDE)], here.to_y),
            )
        if phase == 4:
            return (
                (w.at[c, 0, :, :, :, col(c_x, WIDE)], here.to_x),
                (w.at[c, 1, :, :, :, col(c_y, WIDE)], here.to_y),
                (w.at[c, 2, :, zn, :, col(c_c, HALF)], here.to_zn),
            )
        return ((w.at[c, :, :, :, :, col(c_c, HALF)], here.to_core),)

    def total(phase, c):
        if phase == 1:
            return w.at[c, :, 0, 0, :, 0:LANE]
        if phase == 2:
            return w.at[c, :, :, 0, :, 0:LANE]
        return w.at[c, :, :, :, :, 0 : {3: LANE, 4: WIDE, 5: HALF}[phase]]

    def arrived(phase, c):
        if phase == 0:
            wait_bytes(total(1, c), r0.at[c])
        else:
            slot = c % SLOTS
            wait_bytes(total(phase, c), rsem.at[phase - 1, slot])
            wait_bytes(total(phase, c), ssem.at[phase - 1, slot])

    def advance(phase, c):
        arrived(phase - 1, c)
        slot = c % SLOTS
        for ref, to in parts(phase, c):
            remote(ref, ref, ssem.at[phase - 1, slot], rsem.at[phase - 1, slot], to).start()

    def one_tile(c, i):
        at = pl.ds(pl.multiple_of(i * tile, tile), tile)
        x32 = h[c, at, :].astype(F32)
        inv = lax.rsqrt(jnp.mean(x32 * x32, axis=-1, keepdims=True) + NORM_EPS)
        n = (x32 * inv).astype(BF16)
        acc = x32
        ahead = mat(n, square(w, c, 0, 0)), mat(n, square(w, c, 1, 0))
        for k in range(4):
            a, b = ahead
            if k < 3:
                ahead = mat(n, square(w, c, 0, k + 1)), mat(n, square(w, c, 1, k + 1))
            u = (a * jax.nn.sigmoid(a) * b).astype(BF16)
            acc += mat(u, out_square(w, c, k))
        h[c + 1, at, :] = acc.astype(BF16)

    lead = max(P_AHEAD)

    def step(i, carry):
        for k in (5, 4, 3, 2, 1):
            since = i - lead + P_AHEAD[k]

            @pl.when((since >= 0) & (since < TICKS * n_block) & ((since + TICKS * lead) % TICKS == 0))
            def _(k=k, since=since):
                advance(k, since // TICKS)

        @pl.when(i >= lead)
        def _():
            now = i - lead
            c = now // TICKS

            @pl.when(now % TICKS == 0)
            def _():
                arrived(5, c)

            @pl.when(now % TICKS == 1)
            def _():
                pltpu.make_async_copy(w.at[c], w_all.at[c], wsem.at[c]).start()
                pltpu.make_async_copy(h.at[c], h_all.at[c], hsem.at[c]).start()

            @pl.when(c < n_block - 1)
            def _():
                one_tile(c, now % TICKS)

        return carry

    lax.fori_loop(0, lead, step, 0)
    load.wait()
    lax.fori_loop(lead, lead + TICKS * n_block, step, 0)
    for v in range(n_v):
        wait_bytes(w.at[0, :, 0, 0, :, 0 : LANE * (n_stage - 1)], s0.at[v])

    def drain(c, carry):
        pltpu.make_async_copy(w.at[c], w_all.at[c], wsem.at[c]).wait()
        pltpu.make_async_copy(h.at[c], h_all.at[c], hsem.at[c]).wait()
        return carry

    lax.fori_loop(0, n_block, drain, 0)


def bwd_kernel(n_stage, cot, w_all, h_all, gg, gi, go, ga, w, h, e, g, x1, x2g, x2i, x2o, x3gl, x3il, x3gh, x3ih, x3a, x3b, x4g, x4i, x4a, x4b, x5g, x5i, x5a, x5b, fg, fi, fa, fb, ssem, rsem, own, fsem, wsem, hsem, esem, as_, ar, cs, cr, cl):
    here = Place()
    z, s, zn, zf, x, y, core = here.z, here.s, here.zn, here.zf, here.x, here.y, here.core
    n_block = w_all.shape[0]
    n_v = n_block // n_stage
    rows = h.shape[1]
    tile = rows // TICKS
    c_g, c_i = narrow(core, x, y), narrow(core, y, x)

    load_e = pltpu.make_async_copy(cot.at[s], e.at[s], esem)
    load_e.start()

    def fetch(b):
        c, slot = n_block - 1 - b, b % 2
        return (
            pltpu.make_async_copy(w_all.at[c], w.at[slot], wsem.at[slot]),
            pltpu.make_async_copy(h_all.at[c], h.at[slot], hsem.at[slot]),
        )

    for copy in fetch(0):
        copy.start()
    enter(here, n_stage)
    load_e.wait()

    def total(phase, slot):
        if phase == 1:
            return x1.at[slot]
        if phase == 2:
            return x1.at[slot, :, :, :, :, 0:WIDE]
        if phase == 3:
            return x1.at[slot, :, :, :, :, 0:LANE]
        if phase == 4:
            return x1.at[slot, :, :, 0, :, 0:LANE]
        return x1.at[slot, :, 0, 0, :, 0:LANE]

    def push(phase, b, moves):
        slot = b % SLOTS
        for src, dst, to in moves:
            remote(src, dst, ssem.at[phase - 1, slot], rsem.at[phase - 1, slot], to).start()

    def taken(phase, b):
        slot = b % SLOTS
        wait_bytes(total(phase, slot), rsem.at[phase - 1, slot])
        wait_bytes(total(phase, slot), ssem.at[phase - 1, slot])

    def when_valid(b, fn):
        @pl.when((b >= 0) & (b < n_block))
        def _():
            fn(b)

    def q1(b):
        push(1, b, ((g.at[b % 2, :, :, :, :, col(HALF - HALF * core, HALF)], x1.at[b % SLOTS], here.to_core),))

    def q2(b):
        taken(1, b)
        q, p = b % SLOTS, b % 2
        for m in range(3):
            for f in range(2):
                for k in range(2):
                    x1[q, m, f, k] += g[p, m, f, k, :, col(HALF * core, HALF)]
        push(2, b, (
            (x1.at[q, 0, :, :, :, col(WIDE - WIDE * x, WIDE)], x2g.at[q], here.to_x),
            (x1.at[q, 1, :, :, :, col(WIDE - WIDE * y, WIDE)], x2i.at[q], here.to_y),
            (x1.at[q, 2, :, 1 - zn], x2o.at[q], here.to_zn),
        ))

    def q3(b):
        taken(2, b)
        q = b % SLOTS
        for f in range(2):
            for k in range(2):
                x2g[q, f, k] += x1[q, 0, f, k, :, col(WIDE * x, WIDE)]
                x2i[q, f, k] += x1[q, 1, f, k, :, col(WIDE * y, WIDE)]
            x2o[q, f] += x1[q, 2, f, zn]
        push(3, b, (
            (x2g.at[q, :, :, LO, col(LANE - LANE * y, LANE)], x3gl.at[q], here.to_y),
            (x2i.at[q, :, :, LO, col(LANE - LANE * x, LANE)], x3il.at[q], here.to_x),
            (x2g.at[q, :, 1 - zn, HI], x3gh.at[q], here.to_zn),
            (x2i.at[q, :, 1 - zn, HI], x3ih.at[q], here.to_zn),
            (x2o.at[q, :, LO, col(WIDE - WIDE * x, WIDE)], x3a.at[q], here.to_x),
            (x2o.at[q, :, HI, col(WIDE - WIDE * y, WIDE)], x3b.at[q], here.to_y),
        ))

    def q4(b):
        taken(3, b)
        q = b % SLOTS
        for f in range(2):
            for k in range(2):
                x3gl[q, f, k] += x2g[q, f, k, LO, col(LANE * y, LANE)]
                x3il[q, f, k] += x2i[q, f, k, LO, col(LANE * x, LANE)]
            x3gh[q, f] += x2g[q, f, zn, HI]
            x3ih[q, f] += x2i[q, f, zn, HI]
            x3a[q, f] += x2o[q, f, LO, col(WIDE * x, WIDE)]
            x3b[q, f] += x2o[q, f, HI, col(WIDE * y, WIDE)]
        push(4, b, (
            (x3gl.at[q, :, 1 - zn], x4g.at[q, :, LO], here.to_zn),
            (x3il.at[q, :, 1 - zn], x4i.at[q, :, LO], here.to_zn),
            (x3gh.at[q, :, :, col(LANE - LANE * y, LANE)], x4g.at[q, :, HI], here.to_y),
            (x3ih.at[q, :, :, col(LANE - LANE * x, LANE)], x4i.at[q, :, HI], here.to_x),
            (x3a.at[q, :, :, col(LANE - LANE * y, LANE)], x4a.at[q], here.to_y),
            (x3b.at[q, :, :, col(LANE - LANE * x, LANE)], x4b.at[q], here.to_x),
        ))

    def q5(b):
        taken(4, b)
        q = b % SLOTS
        for f in range(2):
            x4g[q, f, LO] += x3gl[q, f, zn]
            x4i[q, f, LO] += x3il[q, f, zn]
            x4g[q, f, HI] += x3gh[q, f, :, col(LANE * y, LANE)]
            x4i[q, f, HI] += x3ih[q, f, :, col(LANE * x, LANE)]
            x4a[q, f] += x3a[q, f, :, col(LANE * y, LANE)]
            x4b[q, f] += x3b[q, f, :, col(LANE * x, LANE)]
        push(5, b, (
            (x4g.at[q, 1 - zf], x5g.at[q], here.to_zf),
            (x4i.at[q, 1 - zf], x5i.at[q], here.to_zf),
            (x4a.at[q, 1 - zf], x5a.at[q], here.to_zf),
            (x4b.at[q, 1 - zf], x5b.at[q], here.to_zf),
        ))

    def q6(b):
        taken(5, b)
        q = b % SLOTS
        c = n_block - 1 - b
        v, p = c // n_stage, c % n_stage
        fg[b] = x5g[q] + x4g[q, zf]
        fi[b] = x5i[q] + x4i[q, zf]
        fa[b] = x5a[q] + x4a[q, zf]
        fb[b] = x5b[q] + x4b[q, zf]
        moves = (
            (fg.at[b], gg.at[v, 0, :, col(c_g, LANE)]),
            (fi.at[b], gi.at[v, 0, :, col(c_i, LANE)]),
            (fa.at[b], go.at[v, 0, pl.ds(pl.multiple_of(PIECE * (2 * core + x), SUB), SUB), col(LANE * y, LANE)]),
            (fb.at[b], go.at[v, 0, pl.ds(pl.multiple_of(PIECE * (2 * core + y) + SUB, SUB), SUB), col(LANE * x, LANE)]),
        )

        @pl.when(p == s)
        def _():
            for src, dst in moves:
                pltpu.make_async_copy(src, dst, own.at[b]).start()

        @pl.when(p != s)
        def _():
            for src, dst in moves:
                remote(src, dst, own.at[b], fsem.at[v], (z, p)).start()

    def one_tile(b, i):
        at = pl.ds(pl.multiple_of(i * tile, tile), tile)
        p = b % 2
        first = i == 0
        x32 = h[p, at, :].astype(F32)
        inv = lax.rsqrt(jnp.mean(x32 * x32, axis=-1, keepdims=True) + NORM_EPS)
        hr = x32 * inv
        n = hr.astype(BF16)
        et = e[s, at, :]
        q = jnp.zeros((tile, WIDE), F32)

        def add(m, k, value):
            for f in range(2):
                for r in range(2):
                    part = value[LANE * f + PIECE * r : LANE * f + PIECE * r + PIECE]
                    old = g[p, m, f, r, :, WIDE * k : WIDE * k + WIDE]
                    g[p, m, f, r, :, WIDE * k : WIDE * k + WIDE] = part + jnp.where(first, 0.0, old)

        def up(k):
            return mat(n, square(w, p, 0, k)), mat(n, square(w, p, 1, k)), mat_cols(et, out_square(w, p, k))

        ahead = up(0)
        for k in range(4):
            a, bb, t = ahead
            if k < 3:
                ahead = up(k + 1)
            sg = jax.nn.sigmoid(a)
            act = a * sg
            u = (act * bb).astype(BF16)
            da = (t * bb * sg * (1.0 + a * (1.0 - sg))).astype(BF16)
            db = (t * act).astype(BF16)
            q += mat_cols(da, square(w, p, 0, k)) + mat_cols(db, square(w, p, 1, k))
            add(0, k, mat_rows(n, da))
            add(1, k, mat_rows(n, db))
            do = mat_rows(u, et)
            for j in range(4):
                old = g[p, 2, k // 2, k % 2, :, WIDE * j : WIDE * j + WIDE]
                g[p, 2, k // 2, k % 2, :, WIDE * j : WIDE * j + WIDE] = do[PIECE * j : PIECE * j + PIECE] + jnp.where(first, 0.0, old)
        grad = et.astype(F32) + inv * (q - hr * jnp.mean(q * hr, axis=-1, keepdims=True))
        e[s, at, :] = grad.astype(BF16)

    def step(i, carry):
        for k, fn in ((6, q6), (5, q5), (4, q4), (3, q3), (2, q2), (1, q1)):
            since = i - Q_AT[k]

            @pl.when((since >= 0) & (since < TICKS * n_block) & ((since + TICKS * n_block) % TICKS == 0))
            def _(fn=fn, since=since):
                fn(since // TICKS)

        @pl.when(i < TICKS * n_block)
        def _():
            b = i // TICKS

            @pl.when(i % TICKS == 0)
            def _():
                for copy in fetch(b):
                    copy.wait()

                @pl.when(b + 1 < n_block)
                def _():
                    for copy in fetch(b + 1):
                        copy.start()

            one_tile(b, i % TICKS)

        return carry

    half = rows // 2
    lo, hi = pl.ds(0, half), pl.ds(half, half)
    sx, sy = here.to_x[1], here.to_y[1]
    sd = 2 * ((sx // 2 + sy // 2 - s // 2) % (n_stage // 2)) + core

    def share(k, slot, part, to):
        return remote(e.at[slot, part], e.at[slot, part], as_.at[k], ar.at[k], to)

    first = (share(0, s, lo, here.to_x), share(1, s, lo, here.to_y), share(2, s, hi, here.to_y), share(3, s, hi, here.to_x))
    relay = (share(4, sx, lo, here.to_y), share(5, sy, hi, here.to_x))

    def hand(k, slot):
        return (
            remote(e.at[slot], ga.at[slot], cs.at[k], cr.at[k], here.to_core),
            pltpu.make_async_copy(e.at[slot], ga.at[slot], cl.at[k]),
        )

    hands = [hand(k, slot) for k, slot in enumerate((s, sx, sy, sd))]
    last = TICKS * n_block
    lax.fori_loop(0, last - 1, step, 0)
    for copy in first[:2]:
        copy.start()
    lax.fori_loop(last - 1, last, step, 0)
    for copy in first[2:]:
        copy.start()
    lax.fori_loop(last, last + RELAY_AT, step, 0)
    first[0].wait_recv()
    relay[0].start()
    first[2].wait_recv()
    relay[1].start()
    for copy in hands[0]:
        copy.start()
    lax.fori_loop(last + RELAY_AT, last + Q_AT[6], step, 0)
    first[3].wait_recv()
    for copy in hands[1]:
        copy.start()
    first[1].wait_recv()
    for copy in hands[2]:
        copy.start()
    for copy in relay:
        copy.wait_recv()
    for copy in hands[3]:
        copy.start()
    for copy in first + relay:
        copy.wait_send()

    def finish(b, carry):
        wait_bytes(total(5, 0), own.at[b])
        return carry

    lax.fori_loop(0, n_block, finish, 0)
    for v in range(n_v):
        wait_bytes(g.at[0, :, 0, 0, :, 0 : LANE * (n_stage - 1)], fsem.at[v])
    for pair in hands:
        for copy in pair:
            copy.wait()


def settle_kernel(*refs):
    n = (len(refs) - 2) // 3
    srcs, dsts, bufs, (rsem, wsem) = refs[:n], refs[n : 2 * n], refs[2 * n : 3 * n], refs[3 * n :]
    moves = []
    for a in range(n):
        for i in range(srcs[a].shape[0]):
            k = len(moves)
            moves.append((
                pltpu.make_async_copy(srcs[a].at[i], bufs[a].at[i], rsem.at[k]),
                pltpu.make_async_copy(bufs[a].at[i], dsts[a].at[i], wsem.at[k]),
            ))
    for read, _ in moves:
        read.start()
    for read, write in moves:
        read.wait()
        write.start()
    for _, write in moves:
        write.wait()


def solution(mesh):
    n_stage = mesh.shape["stage"]
    act_spec = P(None, "data", None, None)
    w_spec = P(None, "stage", "data", None)
    hbm = pl.BlockSpec(memory_space=pltpu.HBM)
    dma = pltpu.SemaphoreType.DMA

    def body(act_in, cot_out, w_gate, w_in, w_out):
        n_micro, n_seq, n_tok, width = act_in.shape
        n_v, _, _, ffn = w_gate.shape
        n_block = n_v * n_stage
        rows = n_micro // n_stage * n_seq * n_tok
        act = act_in.reshape(n_stage, rows, width)
        cot = cot_out.reshape(n_stage, rows, width)
        block = (3, 2, 2, PIECE, ffn)
        flops = 2 * rows * width * ffn * n_block

        def f32(*shape):
            return pltpu.VMEM(shape, F32)

        w_all, h_all = pl.pallas_call(
            functools.partial(fwd_kernel, n_stage),
            name="forward",
            out_shape=(jax.ShapeDtypeStruct((n_block, *block), BF16), jax.ShapeDtypeStruct((n_block, rows, width), BF16)),
            in_specs=[hbm] * 4,
            out_specs=[hbm] * 2,
            scratch_shapes=[
                pltpu.VMEM((n_block, *block), BF16),
                pltpu.VMEM((n_block, rows, width), BF16),
                dma((n_v,)),
                dma((n_block,)),
                dma((5, SLOTS)),
                dma((5, SLOTS)),
                dma,
                dma((n_block,)),
                dma((n_block,)),
            ],
            compiler_params=pltpu.CompilerParams(collective_id=0, has_side_effects=True, vmem_limit_bytes=63 * 2**20),
            cost_estimate=pl.CostEstimate(flops=3 * flops, bytes_accessed=2**26, transcendentals=0),
        )(act, w_gate, w_in, w_out)
        n = SLOTS
        gg, gi, go, ga = pl.pallas_call(
            functools.partial(bwd_kernel, n_stage),
            name="backward",
            out_shape=(
                jax.ShapeDtypeStruct(w_gate.shape, F32),
                jax.ShapeDtypeStruct(w_in.shape, F32),
                jax.ShapeDtypeStruct(w_out.shape, F32),
                jax.ShapeDtypeStruct((n_stage, rows, width), BF16),
            ),
            in_specs=[hbm] * 3,
            out_specs=[hbm] * 4,
            scratch_shapes=[
                pltpu.VMEM((2, *block), BF16),
                pltpu.VMEM((2, rows, width), BF16),
                pltpu.VMEM((n_stage, rows, width), BF16),
                f32(2, *block),
                f32(n, 3, 2, 2, PIECE, HALF),
                f32(n, 2, 2, PIECE, WIDE),
                f32(n, 2, 2, PIECE, WIDE),
                f32(n, 2, PIECE, HALF),
                f32(n, 2, 2, SUB, LANE),
                f32(n, 2, 2, SUB, LANE),
                f32(n, 2, SUB, WIDE),
                f32(n, 2, SUB, WIDE),
                f32(n, 2, SUB, WIDE),
                f32(n, 2, SUB, WIDE),
                f32(n, 2, PIECE, LANE),
                f32(n, 2, PIECE, LANE),
                f32(n, 2, SUB, LANE),
                f32(n, 2, SUB, LANE),
                f32(n, PIECE, LANE),
                f32(n, PIECE, LANE),
                f32(n, SUB, LANE),
                f32(n, SUB, LANE),
                f32(n_block, PIECE, LANE),
                f32(n_block, PIECE, LANE),
                f32(n_block, SUB, LANE),
                f32(n_block, SUB, LANE),
                dma((5, SLOTS)),
                dma((5, SLOTS)),
                dma((n_block,)),
                dma((n_v,)),
                dma((2,)),
                dma((2,)),
                dma,
                dma((6,)),
                dma((6,)),
                dma((4,)),
                dma((4,)),
                dma((4,)),
            ],
            compiler_params=pltpu.CompilerParams(collective_id=1, has_side_effects=True, vmem_limit_bytes=63 * 2**20),
            cost_estimate=pl.CostEstimate(flops=8 * flops, bytes_accessed=2**26, transcendentals=0),
        )(cot, w_all, h_all)
        done = (ga, gg, gi, go)
        moved = sum(a.shape[0] for a in done)
        ga, gg, gi, go = pl.pallas_call(
            settle_kernel,
            name="settle",
            out_shape=[jax.ShapeDtypeStruct(a.shape, a.dtype) for a in done],
            in_specs=[hbm] * 4,
            out_specs=[hbm] * 4,
            scratch_shapes=[pltpu.VMEM(a.shape, a.dtype) for a in done] + [dma((moved,)), dma((moved,))],
        )(*done)
        return ga.reshape(act_in.shape), gg, gi, go

    return jax.shard_map(body, mesh=mesh, in_specs=(act_spec, act_spec, w_spec, w_spec, w_spec), out_specs=(act_spec, w_spec, w_spec, w_spec), check_vma=False)
```

```python
import functools

import jax
import jax.numpy as jnp
from jax import lax
from jax.experimental import pallas as pl
from jax.experimental.pallas import tpu as pltpu
from jax.sharding import PartitionSpec as P

NORM_EPS = 1e-6
MESH = pl.DeviceIdType.MESH
TICKS = 3
H_SLOTS = 3
F_SLOTS = 6
P_SLOTS = 10
P_AHEAD = (0, 20, 15, 11, 6, 3)
Q_SLOTS = (0, 4, 7, 9, 9, 8)
Q_AT = (0, 3, 5, 10, 18, 26, 36)
SHARE_AT = (-1, 0, 2, 3, 17, 20)
LANE, WIDE, HALF = 128, 256, 512
PIECE, SUB = 64, 32
LO, HI = slice(0, SUB), slice(SUB, PIECE)
F32 = jnp.float32
BF16 = jnp.bfloat16


class Place:
    def __init__(self):
        self.z, self.s = lax.axis_index("data"), lax.axis_index("stage")
        self.core, self.x, self.y = self.s % 2, (self.s // 2) % 2, self.s // 4
        self.zn, self.zf = self.z % 2, self.z // 2
        self.to_x = (self.z, self.s + 2 - 4 * self.x)
        self.to_y = (self.z, self.s + 4 - 8 * self.y)
        self.to_core = (self.z, self.s + 1 - 2 * self.core)
        self.to_zn = (self.z + 1 - 2 * self.zn, self.s)
        self.to_zf = (self.z + 2 - 4 * self.zf, self.s)


def col(start, size):
    return pl.ds(pl.multiple_of(start, LANE), size)


def narrow(core, hi, lo):
    return HALF * core + WIDE * hi + LANE * lo


def remote(src, dst, ssem, rsem, to):
    return pltpu.make_async_remote_copy(src_ref=src, dst_ref=dst, send_sem=ssem, recv_sem=rsem, device_id=to, device_id_type=MESH)


def wait_bytes(ref, sem):
    pltpu.make_async_copy(ref, ref, sem).wait()


def enter(here, n_stage):
    barrier = pltpu.get_barrier_semaphore()
    peers = [(here.z, (here.s + k) % n_stage) for k in range(1, n_stage)] + [here.to_zn, here.to_zf]
    for peer in peers:
        pl.semaphore_signal(barrier, inc=1, device_id=peer, device_id_type=MESH)
    pl.semaphore_wait(barrier, len(peers))


def mat_rows(left, right):
    return lax.dot_general(left, right, (((0,), (0,)), ((), ())), preferred_element_type=F32)


def mat_cols(left, right):
    return lax.dot_general(left, right, (((1,), (1,)), ((), ())), preferred_element_type=F32)


def mat(left, right):
    return jnp.dot(left, right, preferred_element_type=F32)


def square(w_ref, at, m, k):
    return w_ref[at, m, :, :, :, WIDE * k : WIDE * k + WIDE].reshape(WIDE, WIDE)


def out_square(w_ref, at, k):
    return jnp.concatenate([w_ref[at, 2, k // 2, k % 2, :, WIDE * j : WIDE * j + WIDE] for j in range(4)], axis=0)


def step_kernel(n_stage, act, cot, wg, wi, wo, gg, gi, go, ga, h_all, w, h, e, g, x1, x2g, x2i, x2o, x3gl, x3il, x3gh, x3ih, x3a, x3b, x4g, x4i, x4a, x4b, x5g, x5i, x5a, x5b, fg, fi, fa, fb, s0, r0, ps, pr, qs, qr, own, fsem, hsem, esem, as_, ar, cs, cr, cl):
    here = Place()
    z, s, zn, zf, x, y, core = here.z, here.s, here.zn, here.zf, here.x, here.y, here.core
    n_block = w.shape[0]
    n_v = n_block // n_stage
    rows = h.shape[1]
    tile = rows // TICKS
    span = TICKS * n_block
    c_g, c_i = narrow(core, x, y), narrow(core, y, x)
    c_x, c_y, c_c = narrow(core, x, 0), narrow(core, y, 0), narrow(core, 0, 0)

    enter(here, n_stage)
    load_h = pltpu.make_async_copy(act.at[s], h.at[0], esem.at[0])
    load_e = pltpu.make_async_copy(cot.at[s], e.at[0], esem.at[1])
    load_h.start()

    def scatter(v, k):
        q = (s + k) % n_stage
        core, x, y = q % 2, (q // 2) % 2, q // 4
        d_g, d_i = narrow(core, x, y), narrow(core, y, x)
        c = v * n_stage + s
        moves = (
            (wg.at[v, 0, :, col(d_g, LANE)], w.at[c, 0, zf, zn, :, col(d_g, LANE)]),
            (wi.at[v, 0, :, col(d_i, LANE)], w.at[c, 1, zf, zn, :, col(d_i, LANE)]),
            (wo.at[v, 0, pl.ds(pl.multiple_of(PIECE * (2 * core + x), SUB), SUB), col(LANE * y, LANE)], w.at[c, 2, zf, zn, 0:SUB, col(d_g, LANE)]),
            (wo.at[v, 0, pl.ds(pl.multiple_of(PIECE * (2 * core + y) + SUB, SUB), SUB), col(LANE * x, LANE)], w.at[c, 2, zf, zn, SUB:PIECE, col(d_i, LANE)]),
        )
        for src, dst in moves:
            if k == 0:
                pltpu.make_async_copy(src, dst, r0.at[c]).start()
            else:
                remote(src, dst, s0.at[v], r0.at[c], (z, q)).start()

    for v in range(n_v):
        for k in range(n_stage):
            scatter(v, k)
    load_e.start()

    def parts(phase, c):
        if phase == 1:
            return (
                (w.at[c, 0, zf, zn, :, col(c_g, LANE)], here.to_zf),
                (w.at[c, 1, zf, zn, :, col(c_i, LANE)], here.to_zf),
                (w.at[c, 2, zf, zn, 0:SUB, col(c_g, LANE)], here.to_zf),
                (w.at[c, 2, zf, zn, SUB:PIECE, col(c_i, LANE)], here.to_zf),
            )
        if phase == 2:
            return (
                (w.at[c, 0, :, zn, :, col(c_g, LANE)], here.to_zn),
                (w.at[c, 1, :, zn, :, col(c_i, LANE)], here.to_zn),
                (w.at[c, 2, :, zn, 0:SUB, col(c_g, LANE)], here.to_y),
                (w.at[c, 2, :, zn, SUB:PIECE, col(c_i, LANE)], here.to_x),
            )
        if phase == 3:
            return (
                (w.at[c, 0, :, :, :, col(c_g, LANE)], here.to_y),
                (w.at[c, 1, :, :, :, col(c_i, LANE)], here.to_x),
                (w.at[c, 2, :, zn, 0:SUB, col(c_x, WIDE)], here.to_x),
                (w.at[c, 2, :, zn, SUB:PIECE, col(c_y, WIDE)], here.to_y),
            )
        if phase == 4:
            return (
                (w.at[c, 0, :, :, :, col(c_x, WIDE)], here.to_x),
                (w.at[c, 1, :, :, :, col(c_y, WIDE)], here.to_y),
                (w.at[c, 2, :, zn, :, col(c_c, HALF)], here.to_zn),
            )
        return ((w.at[c, :, :, :, :, col(c_c, HALF)], here.to_core),)

    def w_total(phase, c):
        if phase == 1:
            return w.at[c, :, 0, 0, :, 0:LANE]
        if phase == 2:
            return w.at[c, :, :, 0, :, 0:LANE]
        return w.at[c, :, :, :, :, 0 : {3: LANE, 4: WIDE, 5: HALF}[phase]]

    def arrived(phase, c):
        if phase == 0:
            wait_bytes(w_total(1, c), r0.at[c])
        else:
            slot = c % P_SLOTS
            wait_bytes(w_total(phase, c), pr.at[phase - 1, slot])
            wait_bytes(w_total(phase, c), ps.at[phase - 1, slot])

    def advance(phase, c):
        arrived(phase - 1, c)
        slot = c % P_SLOTS
        for ref, to in parts(phase, c):
            remote(ref, ref, ps.at[phase - 1, slot], pr.at[phase - 1, slot], to).start()

    def fwd_tile(c, i):
        at = pl.ds(pl.multiple_of(i * tile, tile), tile)
        x32 = h[c % H_SLOTS, at, :].astype(F32)
        inv = lax.rsqrt(jnp.mean(x32 * x32, axis=-1, keepdims=True) + NORM_EPS)
        n = (x32 * inv).astype(BF16)
        acc = x32
        ahead = mat(n, square(w, c, 0, 0)), mat(n, square(w, c, 1, 0))
        for k in range(4):
            a, b = ahead
            if k < 3:
                ahead = mat(n, square(w, c, 0, k + 1)), mat(n, square(w, c, 1, k + 1))
            u = (a * jax.nn.sigmoid(a) * b).astype(BF16)
            acc += mat(u, out_square(w, c, k))
        h[(c + 1) % H_SLOTS, at, :] = acc.astype(BF16)

    def keep(c):
        return pltpu.make_async_copy(h.at[c % H_SLOTS], h_all.at[c], hsem.at[c])

    def recall(c):
        return pltpu.make_async_copy(h_all.at[c], h.at[c % H_SLOTS], hsem.at[c])

    n_kept = n_block - H_SLOTS
    lead = max(P_AHEAD)

    def lead_step(i, carry):
        for k in (5, 4, 3, 2, 1):
            since = i - lead + P_AHEAD[k]

            @pl.when((since >= 0) & (since < span) & ((since + TICKS * lead) % TICKS == 0))
            def _(k=k, since=since):
                advance(k, since // TICKS)

        return carry

    def fwd_step(i, carry):
        lead_step(i, carry)
        now = i - lead
        c = now // TICKS

        @pl.when(now % TICKS == 0)
        def _():
            arrived(5, c)

            @pl.when((c >= 2) & (c - 2 < n_kept))
            def _():
                keep(c - 2).wait()

        @pl.when((now % TICKS == 1) & (c < n_kept))
        def _():
            keep(c).start()

        @pl.when(c < n_block - 1)
        def _():
            fwd_tile(c, now % TICKS)

        return carry

    lax.fori_loop(0, lead, lead_step, 0)
    load_h.wait()
    lax.fori_loop(lead, lead + span, fwd_step, 0)
    load_e.wait()

    def g_total(phase):
        if phase == 1:
            return x1.at[0]
        if phase == 2:
            return x1.at[0, :, :, :, :, 0:WIDE]
        if phase == 3:
            return x1.at[0, :, :, :, :, 0:LANE]
        if phase == 4:
            return x1.at[0, :, :, 0, :, 0:LANE]
        return x1.at[0, :, 0, 0, :, 0:LANE]

    def slot_of(phase, b):
        return b % Q_SLOTS[phase]

    def push(phase, b, moves):
        slot = slot_of(phase, b)
        for src, dst, to in moves:
            remote(src, dst, qs.at[phase - 1, slot], qr.at[phase - 1, slot], to).start()

    def taken(phase, b):
        slot = slot_of(phase, b)
        wait_bytes(g_total(phase), qr.at[phase - 1, slot])
        wait_bytes(g_total(phase), qs.at[phase - 1, slot])

    def q1(b):
        push(1, b, ((g.at[b % 2, :, :, :, :, col(HALF - HALF * core, HALF)], x1.at[slot_of(1, b)], here.to_core),))

    def q2(b):
        taken(1, b)
        q, t, p = slot_of(1, b), slot_of(2, b), b % 2
        for m in range(3):
            for f in range(2):
                for k in range(2):
                    x1[q, m, f, k] += g[p, m, f, k, :, col(HALF * core, HALF)]
        push(2, b, (
            (x1.at[q, 0, :, :, :, col(WIDE - WIDE * x, WIDE)], x2g.at[t], here.to_x),
            (x1.at[q, 1, :, :, :, col(WIDE - WIDE * y, WIDE)], x2i.at[t], here.to_y),
            (x1.at[q, 2, :, 1 - zn], x2o.at[t], here.to_zn),
        ))

    def q3(b):
        taken(2, b)
        o, q, t = slot_of(1, b), slot_of(2, b), slot_of(3, b)
        for f in range(2):
            for k in range(2):
                x2g[q, f, k] += x1[o, 0, f, k, :, col(WIDE * x, WIDE)]
                x2i[q, f, k] += x1[o, 1, f, k, :, col(WIDE * y, WIDE)]
            x2o[q, f] += x1[o, 2, f, zn]
        push(3, b, (
            (x2g.at[q, :, :, LO, col(LANE - LANE * y, LANE)], x3gl.at[t], here.to_y),
            (x2i.at[q, :, :, LO, col(LANE - LANE * x, LANE)], x3il.at[t], here.to_x),
            (x2g.at[q, :, 1 - zn, HI], x3gh.at[t], here.to_zn),
            (x2i.at[q, :, 1 - zn, HI], x3ih.at[t], here.to_zn),
            (x2o.at[q, :, LO, col(WIDE - WIDE * x, WIDE)], x3a.at[t], here.to_x),
            (x2o.at[q, :, HI, col(WIDE - WIDE * y, WIDE)], x3b.at[t], here.to_y),
        ))

    def q4(b):
        taken(3, b)
        o, q, t = slot_of(2, b), slot_of(3, b), slot_of(4, b)
        for f in range(2):
            for k in range(2):
                x3gl[q, f, k] += x2g[o, f, k, LO, col(LANE * y, LANE)]
                x3il[q, f, k] += x2i[o, f, k, LO, col(LANE * x, LANE)]
            x3gh[q, f] += x2g[o, f, zn, HI]
            x3ih[q, f] += x2i[o, f, zn, HI]
            x3a[q, f] += x2o[o, f, LO, col(WIDE * x, WIDE)]
            x3b[q, f] += x2o[o, f, HI, col(WIDE * y, WIDE)]
        push(4, b, (
            (x3gl.at[q, :, 1 - zn], x4g.at[t, :, LO], here.to_zn),
            (x3il.at[q, :, 1 - zn], x4i.at[t, :, LO], here.to_zn),
            (x3gh.at[q, :, :, col(LANE - LANE * y, LANE)], x4g.at[t, :, HI], here.to_y),
            (x3ih.at[q, :, :, col(LANE - LANE * x, LANE)], x4i.at[t, :, HI], here.to_x),
            (x3a.at[q, :, :, col(LANE - LANE * y, LANE)], x4a.at[t], here.to_y),
            (x3b.at[q, :, :, col(LANE - LANE * x, LANE)], x4b.at[t], here.to_x),
        ))

    def q5(b):
        taken(4, b)
        o, q, t = slot_of(3, b), slot_of(4, b), slot_of(5, b)
        for f in range(2):
            x4g[q, f, LO] += x3gl[o, f, zn]
            x4i[q, f, LO] += x3il[o, f, zn]
            x4g[q, f, HI] += x3gh[o, f, :, col(LANE * y, LANE)]
            x4i[q, f, HI] += x3ih[o, f, :, col(LANE * x, LANE)]
            x4a[q, f] += x3a[o, f, :, col(LANE * y, LANE)]
            x4b[q, f] += x3b[o, f, :, col(LANE * x, LANE)]
        push(5, b, (
            (x4g.at[q, 1 - zf], x5g.at[t], here.to_zf),
            (x4i.at[q, 1 - zf], x5i.at[t], here.to_zf),
            (x4a.at[q, 1 - zf], x5a.at[t], here.to_zf),
            (x4b.at[q, 1 - zf], x5b.at[t], here.to_zf),
        ))

    def q6(b):
        taken(5, b)
        o, q = slot_of(4, b), slot_of(5, b)
        c = n_block - 1 - b
        v, p = c // n_stage, c % n_stage
        t = b % F_SLOTS

        @pl.when(b >= F_SLOTS)
        def _():
            wait_bytes(g_total(5), own.at[t])

        fg[t] = x5g[q] + x4g[o, zf]
        fi[t] = x5i[q] + x4i[o, zf]
        fa[t] = x5a[q] + x4a[o, zf]
        fb[t] = x5b[q] + x4b[o, zf]
        moves = (
            (fg.at[t], gg.at[v, 0, :, col(c_g, LANE)]),
            (fi.at[t], gi.at[v, 0, :, col(c_i, LANE)]),
            (fa.at[t], go.at[v, 0, pl.ds(pl.multiple_of(PIECE * (2 * core + x), SUB), SUB), col(LANE * y, LANE)]),
            (fb.at[t], go.at[v, 0, pl.ds(pl.multiple_of(PIECE * (2 * core + y) + SUB, SUB), SUB), col(LANE * x, LANE)]),
        )

        @pl.when(p == s)
        def _():
            for src, dst in moves:
                pltpu.make_async_copy(src, dst, own.at[t]).start()

        @pl.when(p != s)
        def _():
            for src, dst in moves:
                remote(src, dst, own.at[t], fsem.at[v], (z, p)).start()

    def bwd_tile(b, i):
        at = pl.ds(pl.multiple_of(i * tile, tile), tile)
        p, c = b % 2, n_block - 1 - b
        first = i == 0
        x32 = h[c % H_SLOTS, at, :].astype(F32)
        inv = lax.rsqrt(jnp.mean(x32 * x32, axis=-1, keepdims=True) + NORM_EPS)
        hr = x32 * inv
        n = hr.astype(BF16)
        et = e[0, at, :]
        q = jnp.zeros((tile, WIDE), F32)

        def add(m, k, value):
            for f in range(2):
                for r in range(2):
                    part = value[LANE * f + PIECE * r : LANE * f + PIECE * r + PIECE]
                    old = g[p, m, f, r, :, WIDE * k : WIDE * k + WIDE]
                    g[p, m, f, r, :, WIDE * k : WIDE * k + WIDE] = part + jnp.where(first, 0.0, old)

        def up(k):
            return mat(n, square(w, c, 0, k)), mat(n, square(w, c, 1, k)), mat_cols(et, out_square(w, c, k))

        ahead = up(0)
        for k in range(4):
            a, bb, t = ahead
            if k < 3:
                ahead = up(k + 1)
            sg = jax.nn.sigmoid(a)
            act = a * sg
            u = (act * bb).astype(BF16)
            da = (t * bb * sg * (1.0 + a * (1.0 - sg))).astype(BF16)
            db = (t * act).astype(BF16)
            q += mat_cols(da, square(w, c, 0, k)) + mat_cols(db, square(w, c, 1, k))
            add(0, k, mat_rows(n, da))
            add(1, k, mat_rows(n, db))
            do = mat_rows(u, et)
            for j in range(4):
                old = g[p, 2, k // 2, k % 2, :, WIDE * j : WIDE * j + WIDE]
                g[p, 2, k // 2, k % 2, :, WIDE * j : WIDE * j + WIDE] = do[PIECE * j : PIECE * j + PIECE] + jnp.where(first, 0.0, old)
        grad = et.astype(F32) + inv * (q - hr * jnp.mean(q * hr, axis=-1, keepdims=True))
        e[0, at, :] = grad.astype(BF16)

    def drain_step(i, carry):
        for k, fn in ((6, q6), (5, q5), (4, q4), (3, q3), (2, q2), (1, q1)):
            since = i - Q_AT[k]

            @pl.when((since >= 0) & (since < span) & ((since + span) % TICKS == 0))
            def _(fn=fn, since=since):
                fn(since // TICKS)

        return carry

    def bwd_step(i, carry):
        drain_step(i, carry)
        b = i // TICKS
        c = n_block - 1 - b

        @pl.when(i % TICKS == 0)
        def _():
            @pl.when(c < n_kept)
            def _():
                recall(c).wait()

            @pl.when((c - 2 >= 0) & (c - 2 < n_kept))
            def _():
                recall(c - 2).start()

        bwd_tile(b, i % TICKS)
        return carry

    half = rows // 2
    lo, hi = pl.ds(0, half), pl.ds(half, half)

    def share(k, src, dst, part, to):
        return remote(e.at[src, part], e.at[dst, part], as_.at[k], ar.at[k], to)

    shares = (
        share(0, 0, 1, lo, here.to_x),
        share(1, 0, 2, hi, here.to_y),
        share(2, 0, 2, lo, here.to_y),
        share(3, 0, 1, hi, here.to_x),
        share(4, 2, 3, hi, here.to_x),
        share(5, 1, 3, lo, here.to_y),
    )
    needs = {4: 1, 5: 0}
    at_tick = 0
    for k, share_at in enumerate(SHARE_AT):
        lax.fori_loop(at_tick, span + share_at, bwd_step if share_at <= 0 else drain_step, 0)
        at_tick = span + share_at
        if k in needs:
            shares[needs[k]].wait_recv()
        shares[k].start()
    lax.fori_loop(at_tick, span + max(Q_AT), drain_step, 0)

    own_slots = (s, here.to_x[1], here.to_y[1], 2 * (n_stage // 2 - 1 - s // 2) + core)
    hands = []
    for k, slot in enumerate(own_slots):
        hands.append(remote(e.at[k], ga.at[slot], cs.at[k], cr.at[k], here.to_core))
        hands.append(pltpu.make_async_copy(e.at[k], ga.at[slot], cl.at[k]))
    for k in range(4):
        for j in ((), (3,), (2,), (4, 5))[k]:
            shares[j].wait_recv()
        for copy in hands[2 * k : 2 * k + 2]:
            copy.start()
    for copy in shares:
        copy.wait_send()

    def finish(t, carry):
        wait_bytes(g_total(5), own.at[t])
        return carry

    lax.fori_loop(0, F_SLOTS, finish, 0)
    for v in range(n_v):
        wait_bytes(w.at[0, :, 0, 0, :, 0 : LANE * (n_stage - 1)], s0.at[v])
        wait_bytes(g.at[0, :, 0, 0, :, 0 : LANE * (n_stage - 1)], fsem.at[v])
    for copy in hands:
        copy.wait()


def settle_kernel(*refs):
    n = (len(refs) - 2) // 3
    srcs, dsts, bufs, (rsem, wsem) = refs[:n], refs[n : 2 * n], refs[2 * n : 3 * n], refs[3 * n :]
    moves = []
    for a in range(n):
        for i in range(srcs[a].shape[0]):
            k = len(moves)
            moves.append((
                pltpu.make_async_copy(srcs[a].at[i], bufs[a].at[i], rsem.at[k]),
                pltpu.make_async_copy(bufs[a].at[i], dsts[a].at[i], wsem.at[k]),
            ))
    for read, _ in moves:
        read.start()
    for read, write in moves:
        read.wait()
        write.start()
    for _, write in moves:
        write.wait()


def solution(mesh):
    n_stage = mesh.shape["stage"]
    act_spec = P(None, "data", None, None)
    w_spec = P(None, "stage", "data", None)
    hbm = pl.BlockSpec(memory_space=pltpu.HBM)
    dma = pltpu.SemaphoreType.DMA

    def body(act_in, cot_out, w_gate, w_in, w_out):
        n_micro, n_seq, n_tok, width = act_in.shape
        n_v, _, _, ffn = w_gate.shape
        n_block = n_v * n_stage
        rows = n_micro // n_stage * n_seq * n_tok
        block = (3, 2, 2, PIECE, ffn)
        flops = 2 * rows * width * ffn * n_block

        def f32(*shape):
            return pltpu.VMEM(shape, F32)

        def bf16(*shape):
            return pltpu.VMEM(shape, BF16)

        _, n1, n2, n3, n4, n5 = Q_SLOTS
        results = (
            jax.ShapeDtypeStruct(w_gate.shape, F32),
            jax.ShapeDtypeStruct(w_in.shape, F32),
            jax.ShapeDtypeStruct(w_out.shape, F32),
            jax.ShapeDtypeStruct((n_stage, rows, width), BF16),
        )
        *done, _ = pl.pallas_call(
            functools.partial(step_kernel, n_stage),
            name="step",
            out_shape=(*results, jax.ShapeDtypeStruct((n_block - H_SLOTS, rows, width), BF16)),
            in_specs=[hbm] * 5,
            out_specs=[hbm] * 5,
            scratch_shapes=[
                bf16(n_block, *block),
                bf16(H_SLOTS, rows, width),
                bf16(4, rows, width),
                f32(2, *block),
                f32(n1, 3, 2, 2, PIECE, HALF),
                f32(n2, 2, 2, PIECE, WIDE),
                f32(n2, 2, 2, PIECE, WIDE),
                f32(n2, 2, PIECE, HALF),
                f32(n3, 2, 2, SUB, LANE),
                f32(n3, 2, 2, SUB, LANE),
                f32(n3, 2, SUB, WIDE),
                f32(n3, 2, SUB, WIDE),
                f32(n3, 2, SUB, WIDE),
                f32(n3, 2, SUB, WIDE),
                f32(n4, 2, PIECE, LANE),
                f32(n4, 2, PIECE, LANE),
                f32(n4, 2, SUB, LANE),
                f32(n4, 2, SUB, LANE),
                f32(n5, PIECE, LANE),
                f32(n5, PIECE, LANE),
                f32(n5, SUB, LANE),
                f32(n5, SUB, LANE),
                f32(F_SLOTS, PIECE, LANE),
                f32(F_SLOTS, PIECE, LANE),
                f32(F_SLOTS, SUB, LANE),
                f32(F_SLOTS, SUB, LANE),
                dma((n_v,)),
                dma((n_block,)),
                dma((5, P_SLOTS)),
                dma((5, P_SLOTS)),
                dma((5, max(Q_SLOTS))),
                dma((5, max(Q_SLOTS))),
                dma((F_SLOTS,)),
                dma((n_v,)),
                dma((n_block,)),
                dma((2,)),
                dma((6,)),
                dma((6,)),
                dma((4,)),
                dma((4,)),
                dma((4,)),
            ],
            compiler_params=pltpu.CompilerParams(collective_id=0, has_side_effects=True, vmem_limit_bytes=67_000_000),
            cost_estimate=pl.CostEstimate(flops=11 * flops, bytes_accessed=2**26, transcendentals=0),
        )(act_in.reshape(n_stage, rows, width), cot_out.reshape(n_stage, rows, width), w_gate, w_in, w_out)
        moved = sum(a.shape[0] for a in done)
        gg, gi, go, ga = pl.pallas_call(
            settle_kernel,
            name="settle",
            out_shape=results,
            in_specs=[hbm] * 4,
            out_specs=[hbm] * 4,
            scratch_shapes=[pltpu.VMEM(a.shape, a.dtype) for a in done] + [dma((moved,)), dma((moved,))],
        )(*done)
        return ga.reshape(act_in.shape), gg, gi, go

    return jax.shard_map(body, mesh=mesh, in_specs=(act_spec, act_spec, w_spec, w_spec, w_spec), out_specs=(act_spec, w_spec, w_spec, w_spec), check_vma=False)
```

```python
import functools

import jax
import jax.numpy as jnp
from jax import lax
from jax.experimental import pallas as pl
from jax.experimental.pallas import tpu as pltpu
from jax.sharding import PartitionSpec as P

NORM_EPS = 1e-6
MESH = pl.DeviceIdType.MESH
TICKS = 3
H_SLOTS = 3
F_SLOTS = 6
P_AHEAD = (0, 19, 14, 10, 5, 2)
Q_SLOTS = (0, 4, 7, 9, 9, 8)
Q_AT = (0, 3, 5, 10, 19, 27, 37)
RELAY_AT = 7
HAND_AT = 10
LANE, WIDE, HALF = 128, 256, 512
PIECE, SUB = 64, 32
LO, HI = slice(0, SUB), slice(SUB, PIECE)
MOST, REST = slice(0, 48), slice(48, PIECE)
F32 = jnp.float32
BF16 = jnp.bfloat16


class Place:
    def __init__(self):
        self.z, self.s = lax.axis_index("data"), lax.axis_index("stage")
        self.core, self.x, self.y = self.s % 2, (self.s // 2) % 2, self.s // 4
        self.zn, self.zf = self.z % 2, self.z // 2
        self.to_x = (self.z, self.s + 2 - 4 * self.x)
        self.to_y = (self.z, self.s + 4 - 8 * self.y)
        self.to_core = (self.z, self.s + 1 - 2 * self.core)
        self.to_zn = (self.z + 1 - 2 * self.zn, self.s)
        self.to_zf = (self.z + 2 - 4 * self.zf, self.s)


def col(start, size):
    return pl.ds(pl.multiple_of(start, LANE), size)


def narrow(core, hi, lo):
    return HALF * core + WIDE * hi + LANE * lo


def remote(src, dst, ssem, rsem, to):
    return pltpu.make_async_remote_copy(src_ref=src, dst_ref=dst, send_sem=ssem, recv_sem=rsem, device_id=to, device_id_type=MESH)


def wait_bytes(ref, sem):
    pltpu.make_async_copy(ref, ref, sem).wait()


def enter(here, n_stage):
    barrier = pltpu.get_barrier_semaphore()
    peers = [(here.z, (here.s + k) % n_stage) for k in range(1, n_stage)] + [here.to_zn, here.to_zf]
    for peer in peers:
        pl.semaphore_signal(barrier, inc=1, device_id=peer, device_id_type=MESH)
    pl.semaphore_wait(barrier, len(peers))


def mat_rows(left, right):
    return lax.dot_general(left, right, (((0,), (0,)), ((), ())), preferred_element_type=F32)


def mat_cols(left, right):
    return lax.dot_general(left, right, (((1,), (1,)), ((), ())), preferred_element_type=F32)


def mat(left, right):
    return jnp.dot(left, right, preferred_element_type=F32)


def square(w_ref, at, m, k):
    return w_ref[at, m, :, :, :, WIDE * k : WIDE * k + WIDE].reshape(WIDE, WIDE)


def out_square(w_ref, at, k):
    return jnp.concatenate([w_ref[at, 2, k // 2, k % 2, :, WIDE * j : WIDE * j + WIDE] for j in range(4)], axis=0)


def step_kernel(n_stage, act, cot, wg, wi, wo, gg, gi, go, ga, h_all, w, h, e, g, x1, x2g, x2i, x2o, x3gl, x3il, x3gh, x3ih, x3a, x3b, x4g, x4i, x4a, x4b, x5g, x5i, x5a, x5b, fg, fi, fa, fb, s0, r0, ps, pr, qs, qr, own, fsem, hsem, esem, as_, ar, cs, cr, cl):
    here = Place()
    z, s, zn, zf, x, y, core = here.z, here.s, here.zn, here.zf, here.x, here.y, here.core
    n_block = w.shape[0]
    n_v = n_block // n_stage
    rows = h.shape[1]
    tile = rows // TICKS
    c_g, c_i = narrow(core, x, y), narrow(core, y, x)
    c_x, c_y, c_c = narrow(core, x, 0), narrow(core, y, 0), narrow(core, 0, 0)

    enter(here, n_stage)
    load_h = pltpu.make_async_copy(act.at[s], h.at[0], esem.at[0])
    load_e = pltpu.make_async_copy(cot.at[s], e.at[0], esem.at[1])
    load_h.start()

    def scatter(v, k):
        q = (s + k) % n_stage
        core, x, y = q % 2, (q // 2) % 2, q // 4
        d_g, d_i = narrow(core, x, y), narrow(core, y, x)
        c = v * n_stage + s
        moves = (
            (wg.at[v, 0, :, col(d_g, LANE)], w.at[c, 0, zf, zn, :, col(d_g, LANE)]),
            (wi.at[v, 0, :, col(d_i, LANE)], w.at[c, 1, zf, zn, :, col(d_i, LANE)]),
            (wo.at[v, 0, pl.ds(pl.multiple_of(PIECE * (2 * core + x), SUB), SUB), col(LANE * y, LANE)], w.at[c, 2, zf, zn, 0:SUB, col(d_g, LANE)]),
            (wo.at[v, 0, pl.ds(pl.multiple_of(PIECE * (2 * core + y) + SUB, SUB), SUB), col(LANE * x, LANE)], w.at[c, 2, zf, zn, SUB:PIECE, col(d_i, LANE)]),
        )
        for src, dst in moves:
            if k == 0:
                pltpu.make_async_copy(src, dst, r0.at[c]).start()
            else:
                remote(src, dst, s0.at[v], r0.at[c], (z, q)).start()

    for v in range(n_v):
        for k in range(n_stage):
            scatter(v, k)
    load_e.start()

    def parts(phase, c):
        if phase == 1:
            return (
                (w.at[c, 0, zf, zn, :, col(c_g, LANE)], here.to_zf),
                (w.at[c, 1, zf, zn, :, col(c_i, LANE)], here.to_zf),
                (w.at[c, 2, zf, zn, 0:SUB, col(c_g, LANE)], here.to_zf),
                (w.at[c, 2, zf, zn, SUB:PIECE, col(c_i, LANE)], here.to_zf),
            )
        if phase == 2:
            return (
                (w.at[c, 0, :, zn, MOST, col(c_g, LANE)], here.to_zn),
                (w.at[c, 0, :, zn, REST, col(c_g, LANE)], here.to_y),
                (w.at[c, 1, :, zn, MOST, col(c_i, LANE)], here.to_zn),
                (w.at[c, 1, :, zn, REST, col(c_i, LANE)], here.to_x),
                (w.at[c, 2, :, zn, 0:SUB, col(c_g, LANE)], here.to_y),
                (w.at[c, 2, :, zn, SUB:PIECE, col(c_i, LANE)], here.to_x),
            )
        if phase == 3:
            return (
                (w.at[c, 0, :, :, MOST, col(c_g, LANE)], here.to_y),
                (w.at[c, 0, :, zn, REST, col(c_x, WIDE)], here.to_zn),
                (w.at[c, 1, :, :, MOST, col(c_i, LANE)], here.to_x),
                (w.at[c, 1, :, zn, REST, col(c_y, WIDE)], here.to_zn),
                (w.at[c, 2, :, zn, 0:SUB, col(c_x, WIDE)], here.to_x),
                (w.at[c, 2, :, zn, SUB:PIECE, col(c_y, WIDE)], here.to_y),
            )
        if phase == 4:
            return (
                (w.at[c, 0, :, :, :, col(c_x, WIDE)], here.to_x),
                (w.at[c, 1, :, :, :, col(c_y, WIDE)], here.to_y),
                (w.at[c, 2, :, zn, :, col(c_c, HALF)], here.to_zn),
            )
        return ((w.at[c, :, :, :, :, col(c_c, HALF)], here.to_core),)

    def w_total(phase, c):
        if phase == 1:
            return w.at[c, :, 0, 0, :, 0:LANE]
        if phase == 2:
            return w.at[c, :, :, 0, :, 0:LANE]
        return w.at[c, :, :, :, :, 0 : {3: LANE, 4: WIDE, 5: HALF}[phase]]

    def arrived(phase, c):
        if phase == 0:
            wait_bytes(w_total(1, c), r0.at[c])
        else:
            wait_bytes(w_total(phase, c), pr.at[phase - 1, c])
            wait_bytes(w_total(phase, c), ps.at[phase - 1, c])

    def advance(phase, c):
        arrived(phase - 1, c)
        for ref, to in parts(phase, c):
            remote(ref, ref, ps.at[phase - 1, c], pr.at[phase - 1, c], to).start()

    def fwd_tile(c, i):
        at = slice(i * tile, i * tile + tile)
        x32 = h[c % H_SLOTS, at, :].astype(F32)
        inv = lax.rsqrt(jnp.mean(x32 * x32, axis=-1, keepdims=True) + NORM_EPS)
        n = (x32 * inv).astype(BF16)
        acc = x32
        ahead = mat(n, square(w, c, 0, 0)), mat(n, square(w, c, 1, 0))
        for k in range(4):
            a, b = ahead
            if k < 3:
                ahead = mat(n, square(w, c, 0, k + 1)), mat(n, square(w, c, 1, k + 1))
            u = (a * jax.nn.sigmoid(a) * b).astype(BF16)
            acc += mat(u, out_square(w, c, k))
        h[(c + 1) % H_SLOTS, at, :] = acc.astype(BF16)

    def keep(c):
        return pltpu.make_async_copy(h.at[c % H_SLOTS], h_all.at[c], hsem.at[c])

    def recall(c):
        return pltpu.make_async_copy(h_all.at[c], h.at[c % H_SLOTS], hsem.at[c])

    n_kept = n_block - H_SLOTS
    lead = (max(P_AHEAD) + TICKS - 1) // TICKS

    def gather(j, r):
        for k in (5, 4, 3, 2, 1):
            if (P_AHEAD[k] + r) % TICKS == 0:
                c = j + (P_AHEAD[k] + r) // TICKS

                @pl.when((c >= 0) & (c < n_block))
                def _(k=k, c=c):
                    advance(k, c)

    def lead_step(i, carry):
        for r in range(TICKS):
            gather(i - lead, r)
        return carry

    def fwd_step(c, carry):
        for r in range(TICKS):
            gather(c, r)
            if r == 0:
                arrived(5, c)

                @pl.when((c >= 2) & (c - 2 < n_kept))
                def _():
                    keep(c - 2).wait()

            if r == 1:

                @pl.when(c < n_kept)
                def _():
                    keep(c).start()

            fwd_tile(c, r)
        return carry

    lax.fori_loop(0, lead, lead_step, 0)
    load_h.wait()
    lax.fori_loop(0, n_block - 1, fwd_step, 0)
    arrived(5, n_block - 1)
    load_e.wait()

    def g_total(phase):
        if phase == 1:
            return x1.at[0]
        if phase == 2:
            return x1.at[0, :, :, :, :, 0:WIDE]
        if phase == 3:
            return x1.at[0, :, :, :, :, 0:LANE]
        if phase == 4:
            return x1.at[0, :, :, 0, :, 0:LANE]
        return x1.at[0, :, 0, 0, :, 0:LANE]

    def slot_of(phase, b):
        return b % Q_SLOTS[phase]

    def push(phase, b, moves):
        slot = slot_of(phase, b)
        for src, dst, to in moves:
            remote(src, dst, qs.at[phase - 1, slot], qr.at[phase - 1, slot], to).start()

    def taken(phase, b):
        slot = slot_of(phase, b)
        wait_bytes(g_total(phase), qr.at[phase - 1, slot])
        wait_bytes(g_total(phase), qs.at[phase - 1, slot])

    def q1(b):
        push(1, b, ((g.at[b % 2, :, :, :, :, col(HALF - HALF * core, HALF)], x1.at[slot_of(1, b)], here.to_core),))

    def q2(b):
        taken(1, b)
        q, t, p = slot_of(1, b), slot_of(2, b), b % 2
        for m in range(3):
            for f in range(2):
                for k in range(2):
                    x1[q, m, f, k] += g[p, m, f, k, :, col(HALF * core, HALF)]
        push(2, b, (
            (x1.at[q, 0, :, :, :, col(WIDE - WIDE * x, WIDE)], x2g.at[t], here.to_x),
            (x1.at[q, 1, :, :, :, col(WIDE - WIDE * y, WIDE)], x2i.at[t], here.to_y),
            (x1.at[q, 2, :, 1 - zn], x2o.at[t], here.to_zn),
        ))

    def q3(b):
        taken(2, b)
        o, q, t = slot_of(1, b), slot_of(2, b), slot_of(3, b)
        for f in range(2):
            for k in range(2):
                x2g[q, f, k] += x1[o, 0, f, k, :, col(WIDE * x, WIDE)]
                x2i[q, f, k] += x1[o, 1, f, k, :, col(WIDE * y, WIDE)]
            x2o[q, f] += x1[o, 2, f, zn]
        push(3, b, (
            (x2g.at[q, :, :, LO, col(LANE - LANE * y, LANE)], x3gl.at[t], here.to_y),
            (x2i.at[q, :, :, LO, col(LANE - LANE * x, LANE)], x3il.at[t], here.to_x),
            (x2g.at[q, :, 1 - zn, HI], x3gh.at[t], here.to_zn),
            (x2i.at[q, :, 1 - zn, HI], x3ih.at[t], here.to_zn),
            (x2o.at[q, :, LO, col(WIDE - WIDE * x, WIDE)], x3a.at[t], here.to_x),
            (x2o.at[q, :, HI, col(WIDE - WIDE * y, WIDE)], x3b.at[t], here.to_y),
        ))

    def q4(b):
        taken(3, b)
        o, q, t = slot_of(2, b), slot_of(3, b), slot_of(4, b)
        for f in range(2):
            for k in range(2):
                x3gl[q, f, k] += x2g[o, f, k, LO, col(LANE * y, LANE)]
                x3il[q, f, k] += x2i[o, f, k, LO, col(LANE * x, LANE)]
            x3gh[q, f] += x2g[o, f, zn, HI]
            x3ih[q, f] += x2i[o, f, zn, HI]
            x3a[q, f] += x2o[o, f, LO, col(WIDE * x, WIDE)]
            x3b[q, f] += x2o[o, f, HI, col(WIDE * y, WIDE)]
        push(4, b, (
            (x3gl.at[q, :, 1 - zn], x4g.at[t, :, LO], here.to_zn),
            (x3il.at[q, :, 1 - zn], x4i.at[t, :, LO], here.to_zn),
            (x3gh.at[q, :, :, col(LANE - LANE * y, LANE)], x4g.at[t, :, HI], here.to_y),
            (x3ih.at[q, :, :, col(LANE - LANE * x, LANE)], x4i.at[t, :, HI], here.to_x),
            (x3a.at[q, :, :, col(LANE - LANE * y, LANE)], x4a.at[t], here.to_y),
            (x3b.at[q, :, :, col(LANE - LANE * x, LANE)], x4b.at[t], here.to_x),
        ))

    def q5(b):
        taken(4, b)
        o, q, t = slot_of(3, b), slot_of(4, b), slot_of(5, b)
        for f in range(2):
            x4g[q, f, LO] += x3gl[o, f, zn]
            x4i[q, f, LO] += x3il[o, f, zn]
            x4g[q, f, HI] += x3gh[o, f, :, col(LANE * y, LANE)]
            x4i[q, f, HI] += x3ih[o, f, :, col(LANE * x, LANE)]
            x4a[q, f] += x3a[o, f, :, col(LANE * y, LANE)]
            x4b[q, f] += x3b[o, f, :, col(LANE * x, LANE)]
        push(5, b, (
            (x4g.at[q, 1 - zf], x5g.at[t], here.to_zf),
            (x4i.at[q, 1 - zf], x5i.at[t], here.to_zf),
            (x4a.at[q, 1 - zf], x5a.at[t], here.to_zf),
            (x4b.at[q, 1 - zf], x5b.at[t], here.to_zf),
        ))

    def q6(b):
        taken(5, b)
        o, q = slot_of(4, b), slot_of(5, b)
        c = n_block - 1 - b
        v, p = c // n_stage, c % n_stage
        t = b % F_SLOTS

        @pl.when(b >= F_SLOTS)
        def _():
            wait_bytes(g_total(5), own.at[t])

        fg[t] = x5g[q] + x4g[o, zf]
        fi[t] = x5i[q] + x4i[o, zf]
        fa[t] = x5a[q] + x4a[o, zf]
        fb[t] = x5b[q] + x4b[o, zf]
        moves = (
            (fg.at[t], gg.at[v, 0, :, col(c_g, LANE)]),
            (fi.at[t], gi.at[v, 0, :, col(c_i, LANE)]),
            (fa.at[t], go.at[v, 0, pl.ds(pl.multiple_of(PIECE * (2 * core + x), SUB), SUB), col(LANE * y, LANE)]),
            (fb.at[t], go.at[v, 0, pl.ds(pl.multiple_of(PIECE * (2 * core + y) + SUB, SUB), SUB), col(LANE * x, LANE)]),
        )

        @pl.when(p == s)
        def _():
            for src, dst in moves:
                pltpu.make_async_copy(src, dst, own.at[t]).start()

        @pl.when(p != s)
        def _():
            for src, dst in moves:
                remote(src, dst, own.at[t], fsem.at[v], (z, p)).start()

    def bwd_tile(b, i):
        at = slice(i * tile, i * tile + tile)
        p, c = b % 2, n_block - 1 - b
        x32 = h[c % H_SLOTS, at, :].astype(F32)
        inv = lax.rsqrt(jnp.mean(x32 * x32, axis=-1, keepdims=True) + NORM_EPS)
        hr = x32 * inv
        n = hr.astype(BF16)
        et = e[0, at, :]
        q = jnp.zeros((tile, WIDE), F32)

        def add(m, k, value):
            for f in range(2):
                for r in range(2):
                    part = value[LANE * f + PIECE * r : LANE * f + PIECE * r + PIECE]
                    if i > 0:
                        part += g[p, m, f, r, :, WIDE * k : WIDE * k + WIDE]
                    g[p, m, f, r, :, WIDE * k : WIDE * k + WIDE] = part

        def up(k):
            return mat(n, square(w, c, 0, k)), mat(n, square(w, c, 1, k)), mat_cols(et, out_square(w, c, k))

        ahead = up(0)
        for k in range(4):
            a, bb, t = ahead
            if k < 3:
                ahead = up(k + 1)
            sg = jax.nn.sigmoid(a)
            act = a * sg
            u = (act * bb).astype(BF16)
            da = (t * bb * sg * (1.0 + a * (1.0 - sg))).astype(BF16)
            db = (t * act).astype(BF16)
            q += mat_cols(da, square(w, c, 0, k)) + mat_cols(db, square(w, c, 1, k))
            add(0, k, mat_rows(n, da))
            add(1, k, mat_rows(n, db))
            do = mat_rows(u, et)
            for j in range(4):
                part = do[PIECE * j : PIECE * j + PIECE]
                if i > 0:
                    part += g[p, 2, k // 2, k % 2, :, WIDE * j : WIDE * j + WIDE]
                g[p, 2, k // 2, k % 2, :, WIDE * j : WIDE * j + WIDE] = part
        grad = et.astype(F32) + inv * (q - hr * jnp.mean(q * hr, axis=-1, keepdims=True))
        e[0, at, :] = grad.astype(BF16)

    def scatter_sums(j, r):
        for k, fn in ((6, q6), (5, q5), (4, q4), (3, q3), (2, q2), (1, q1)):
            if Q_AT[k] % TICKS == r:
                b = j - Q_AT[k] // TICKS

                @pl.when((b >= 0) & (b < n_block))
                def _(fn=fn, b=b):
                    fn(b)

    def drain_step(j, carry):
        for r in range(TICKS):
            scatter_sums(j, r)
        return carry

    def bwd_step(b, carry):
        c = n_block - 1 - b
        for r in range(TICKS):
            scatter_sums(b, r)
            if r == 0:

                @pl.when(c < n_kept)
                def _():
                    recall(c).wait()

                @pl.when((c - 2 >= 0) & (c - 2 < n_kept))
                def _():
                    recall(c - 2).start()

            bwd_tile(b, r)
        return carry

    half = rows // 2
    lo, hi = pl.ds(0, half), pl.ds(half, half)

    def share(k, src, dst, part, to):
        return remote(e.at[src, part], e.at[dst, part], as_.at[k], ar.at[k], to)

    shares = (
        share(0, 0, 1, lo, here.to_x),
        share(1, 0, 2, lo, here.to_y),
        share(2, 0, 2, hi, here.to_y),
        share(3, 0, 1, hi, here.to_x),
        share(4, 1, 3, lo, here.to_y),
        share(5, 2, 3, hi, here.to_x),
    )
    needs = {4: 0, 5: 2}
    own_slots = (s, here.to_x[1], here.to_y[1], 2 * (n_stage // 2 - 1 - s // 2) + core)
    hands = []
    for k, slot in enumerate(own_slots):
        hands.append(remote(e.at[k], ga.at[slot], cs.at[k], cr.at[k], here.to_core))
        hands.append(pltpu.make_async_copy(e.at[k], ga.at[slot], cl.at[k]))

    def hand(k):
        for copy in hands[2 * k : 2 * k + 2]:
            copy.start()

    lax.fori_loop(0, n_block, bwd_step, 0)
    for copy in shares[:4]:
        copy.start()
    hand(0)
    lax.fori_loop(n_block, n_block + RELAY_AT, drain_step, 0)
    for k in needs:
        shares[needs[k]].wait_recv()
        shares[k].start()
    lax.fori_loop(n_block + RELAY_AT, n_block + HAND_AT, drain_step, 0)
    shares[3].wait_recv()
    hand(1)
    shares[1].wait_recv()
    hand(2)
    lax.fori_loop(n_block + HAND_AT, n_block + max(Q_AT) // TICKS + 1, drain_step, 0)
    shares[4].wait_recv()
    shares[5].wait_recv()
    hand(3)
    for copy in shares:
        copy.wait_send()

    def finish(t, carry):
        wait_bytes(g_total(5), own.at[t])
        return carry

    lax.fori_loop(0, F_SLOTS, finish, 0)
    for v in range(n_v):
        wait_bytes(w.at[0, :, 0, 0, :, 0 : LANE * (n_stage - 1)], s0.at[v])
        wait_bytes(g.at[0, :, 0, 0, :, 0 : LANE * (n_stage - 1)], fsem.at[v])
    for copy in hands:
        copy.wait()


def settle_kernel(*refs):
    n = (len(refs) - 2) // 3
    srcs, dsts, bufs, (rsem, wsem) = refs[:n], refs[n : 2 * n], refs[2 * n : 3 * n], refs[3 * n :]
    moves = []
    for a in range(n):
        for i in range(srcs[a].shape[0]):
            k = len(moves)
            moves.append((
                pltpu.make_async_copy(srcs[a].at[i], bufs[a].at[i], rsem.at[k]),
                pltpu.make_async_copy(bufs[a].at[i], dsts[a].at[i], wsem.at[k]),
            ))
    for read, _ in moves:
        read.start()
    for read, write in moves:
        read.wait()
        write.start()
    for _, write in moves:
        write.wait()


def solution(mesh):
    n_stage = mesh.shape["stage"]
    act_spec = P(None, "data", None, None)
    w_spec = P(None, "stage", "data", None)
    hbm = pl.BlockSpec(memory_space=pltpu.HBM)
    dma = pltpu.SemaphoreType.DMA

    def body(act_in, cot_out, w_gate, w_in, w_out):
        n_micro, n_seq, n_tok, width = act_in.shape
        n_v, _, _, ffn = w_gate.shape
        n_block = n_v * n_stage
        rows = n_micro // n_stage * n_seq * n_tok
        block = (3, 2, 2, PIECE, ffn)
        flops = 2 * rows * width * ffn * n_block

        def f32(*shape):
            return pltpu.VMEM(shape, F32)

        def bf16(*shape):
            return pltpu.VMEM(shape, BF16)

        _, n1, n2, n3, n4, n5 = Q_SLOTS
        results = (
            jax.ShapeDtypeStruct(w_gate.shape, F32),
            jax.ShapeDtypeStruct(w_in.shape, F32),
            jax.ShapeDtypeStruct(w_out.shape, F32),
            jax.ShapeDtypeStruct((n_stage, rows, width), BF16),
        )
        *done, _ = pl.pallas_call(
            functools.partial(step_kernel, n_stage),
            name="step",
            out_shape=(*results, jax.ShapeDtypeStruct((n_block - H_SLOTS, rows, width), BF16)),
            in_specs=[hbm] * 5,
            out_specs=[hbm] * 5,
            scratch_shapes=[
                bf16(n_block, *block),
                bf16(H_SLOTS, rows, width),
                bf16(4, rows, width),
                f32(2, *block),
                f32(n1, 3, 2, 2, PIECE, HALF),
                f32(n2, 2, 2, PIECE, WIDE),
                f32(n2, 2, 2, PIECE, WIDE),
                f32(n2, 2, PIECE, HALF),
                f32(n3, 2, 2, SUB, LANE),
                f32(n3, 2, 2, SUB, LANE),
                f32(n3, 2, SUB, WIDE),
                f32(n3, 2, SUB, WIDE),
                f32(n3, 2, SUB, WIDE),
                f32(n3, 2, SUB, WIDE),
                f32(n4, 2, PIECE, LANE),
                f32(n4, 2, PIECE, LANE),
                f32(n4, 2, SUB, LANE),
                f32(n4, 2, SUB, LANE),
                f32(n5, PIECE, LANE),
                f32(n5, PIECE, LANE),
                f32(n5, SUB, LANE),
                f32(n5, SUB, LANE),
                f32(F_SLOTS, PIECE, LANE),
                f32(F_SLOTS, PIECE, LANE),
                f32(F_SLOTS, SUB, LANE),
                f32(F_SLOTS, SUB, LANE),
                dma((n_v,)),
                dma((n_block,)),
                dma((5, n_block)),
                dma((5, n_block)),
                dma((5, max(Q_SLOTS))),
                dma((5, max(Q_SLOTS))),
                dma((F_SLOTS,)),
                dma((n_v,)),
                dma((n_block,)),
                dma((2,)),
                dma((6,)),
                dma((6,)),
                dma((4,)),
                dma((4,)),
                dma((4,)),
            ],
            compiler_params=pltpu.CompilerParams(collective_id=0, has_side_effects=True, vmem_limit_bytes=67_000_000),
            cost_estimate=pl.CostEstimate(flops=11 * flops, bytes_accessed=2**26, transcendentals=0),
        )(act_in.reshape(n_stage, rows, width), cot_out.reshape(n_stage, rows, width), w_gate, w_in, w_out)
        moved = sum(a.shape[0] for a in done)
        gg, gi, go, ga = pl.pallas_call(
            settle_kernel,
            name="settle",
            out_shape=results,
            in_specs=[hbm] * 4,
            out_specs=[hbm] * 4,
            scratch_shapes=[pltpu.VMEM(a.shape, a.dtype) for a in done] + [dma((moved,)), dma((moved,))],
        )(*done)
        return ga.reshape(act_in.shape), gg, gi, go

    return jax.shard_map(body, mesh=mesh, in_specs=(act_spec, act_spec, w_spec, w_spec, w_spec), out_specs=(act_spec, w_spec, w_spec, w_spec), check_vma=False)
```

```python
import functools

import jax
import jax.numpy as jnp
from jax import lax
from jax.experimental import pallas as pl
from jax.experimental.pallas import tpu as pltpu
from jax.sharding import PartitionSpec as P

NORM_EPS = 1e-6
MESH = pl.DeviceIdType.MESH
TICKS = 3
H_SLOTS = 3
F_SLOTS = 6
P_AHEAD = (0, 19, 14, 10, 5, 2)
Q_SLOTS = (0, 4, 7, 9, 9, 8)
Q_AT = (0, 3, 5, 10, 19, 27, 37)
RELAY_AT = 7
HAND_AT = 10
LANE, WIDE, HALF = 128, 256, 512
PIECE, SUB = 64, 32
LO, HI = slice(0, SUB), slice(SUB, PIECE)
F32 = jnp.float32
BF16 = jnp.bfloat16


class Place:
    def __init__(self):
        self.z, self.s = lax.axis_index("data"), lax.axis_index("stage")
        self.core, self.x, self.y = self.s % 2, (self.s // 2) % 2, self.s // 4
        self.zn, self.zf = self.z % 2, self.z // 2
        self.to_x = (self.z, self.s + 2 - 4 * self.x)
        self.to_y = (self.z, self.s + 4 - 8 * self.y)
        self.to_core = (self.z, self.s + 1 - 2 * self.core)
        self.to_zn = (self.z + 1 - 2 * self.zn, self.s)
        self.to_zf = (self.z + 2 - 4 * self.zf, self.s)


def col(start, size):
    return pl.ds(pl.multiple_of(start, LANE), size)


def narrow(core, hi, lo):
    return HALF * core + WIDE * hi + LANE * lo


def remote(src, dst, ssem, rsem, to):
    return pltpu.make_async_remote_copy(src_ref=src, dst_ref=dst, send_sem=ssem, recv_sem=rsem, device_id=to, device_id_type=MESH)


def wait_bytes(ref, sem):
    pltpu.make_async_copy(ref, ref, sem).wait()


def enter(here, n_stage):
    barrier = pltpu.get_barrier_semaphore()
    peers = [(here.z, (here.s + k) % n_stage) for k in range(1, n_stage)] + [here.to_zn, here.to_zf]
    for peer in peers:
        pl.semaphore_signal(barrier, inc=1, device_id=peer, device_id_type=MESH)
    pl.semaphore_wait(barrier, len(peers))


def mat_rows(left, right):
    return lax.dot_general(left, right, (((0,), (0,)), ((), ())), preferred_element_type=F32)


def mat_cols(left, right):
    return lax.dot_general(left, right, (((1,), (1,)), ((), ())), preferred_element_type=F32)


def mat(left, right):
    return jnp.dot(left, right, preferred_element_type=F32)


def square(w_ref, at, m, k):
    return w_ref[at, m, :, :, :, WIDE * k : WIDE * k + WIDE].reshape(WIDE, WIDE)


def out_square(w_ref, at, k):
    return jnp.concatenate([w_ref[at, 2, k // 2, k % 2, :, WIDE * j : WIDE * j + WIDE] for j in range(4)], axis=0)


def step_kernel(n_stage, act, cot, wg, wi, wo, gg, gi, go, ga, h_all, w, h, e, g, x1, x2g, x2i, x2o, x3gl, x3il, x3gh, x3ih, x3a, x3b, x4g, x4i, x4a, x4b, x5g, x5i, x5a, x5b, fg, fi, fa, fb, s0, r0, ps, pr, qs, qr, own, fsem, hsem, esem, as_, ar, cs, cr, cl):
    here = Place()
    z, s, zn, zf, x, y, core = here.z, here.s, here.zn, here.zf, here.x, here.y, here.core
    n_block = w.shape[0]
    n_v = n_block // n_stage
    rows = h.shape[1]
    tile = rows // TICKS
    c_g, c_i = narrow(core, x, y), narrow(core, y, x)
    c_x, c_y, c_c = narrow(core, x, 0), narrow(core, y, 0), narrow(core, 0, 0)

    enter(here, n_stage)
    load_h = pltpu.make_async_copy(act.at[s], h.at[0], esem.at[0])
    load_e = pltpu.make_async_copy(cot.at[s], e.at[0], esem.at[1])
    load_h.start()

    def scatter(v, k):
        q = (s + k) % n_stage
        core, x, y = q % 2, (q // 2) % 2, q // 4
        d_g, d_i = narrow(core, x, y), narrow(core, y, x)
        c = v * n_stage + s
        moves = (
            (wg.at[v, 0, :, col(d_g, LANE)], w.at[c, 0, zf, zn, :, col(d_g, LANE)]),
            (wi.at[v, 0, :, col(d_i, LANE)], w.at[c, 1, zf, zn, :, col(d_i, LANE)]),
            (wo.at[v, 0, pl.ds(pl.multiple_of(PIECE * (2 * core + x), SUB), SUB), col(LANE * y, LANE)], w.at[c, 2, zf, zn, 0:SUB, col(d_g, LANE)]),
            (wo.at[v, 0, pl.ds(pl.multiple_of(PIECE * (2 * core + y) + SUB, SUB), SUB), col(LANE * x, LANE)], w.at[c, 2, zf, zn, SUB:PIECE, col(d_i, LANE)]),
        )
        for src, dst in moves:
            if k == 0:
                pltpu.make_async_copy(src, dst, r0.at[c]).start()
            else:
                remote(src, dst, s0.at[v], r0.at[c], (z, q)).start()

    for v in range(n_v):
        for k in range(n_stage):
            scatter(v, k)
    load_e.start()

    def parts(phase, c):
        if phase == 1:
            return (
                (w.at[c, 0, zf, zn, :, col(c_g, LANE)], here.to_zf),
                (w.at[c, 1, zf, zn, :, col(c_i, LANE)], here.to_zf),
                (w.at[c, 2, zf, zn, 0:SUB, col(c_g, LANE)], here.to_zf),
                (w.at[c, 2, zf, zn, SUB:PIECE, col(c_i, LANE)], here.to_zf),
            )
        if phase == 2:
            return (
                (w.at[c, 0, :, zn, :, col(c_g, LANE)], here.to_zn),
                (w.at[c, 1, :, zn, :, col(c_i, LANE)], here.to_zn),
                (w.at[c, 2, :, zn, 0:SUB, col(c_g, LANE)], here.to_y),
                (w.at[c, 2, :, zn, SUB:PIECE, col(c_i, LANE)], here.to_x),
            )
        if phase == 3:
            return (
                (w.at[c, 0, :, :, :, col(c_g, LANE)], here.to_y),
                (w.at[c, 1, :, :, :, col(c_i, LANE)], here.to_x),
                (w.at[c, 2, :, zn, 0:SUB, col(c_x, WIDE)], here.to_x),
                (w.at[c, 2, :, zn, SUB:PIECE, col(c_y, WIDE)], here.to_y),
            )
        if phase == 4:
            return (
                (w.at[c, 0, :, :, :, col(c_x, WIDE)], here.to_x),
                (w.at[c, 1, :, :, :, col(c_y, WIDE)], here.to_y),
                (w.at[c, 2, :, zn, :, col(c_c, HALF)], here.to_zn),
            )
        return ((w.at[c, :, :, :, :, col(c_c, HALF)], here.to_core),)

    def w_total(phase, c):
        if phase == 1:
            return w.at[c, :, 0, 0, :, 0:LANE]
        if phase == 2:
            return w.at[c, :, :, 0, :, 0:LANE]
        return w.at[c, :, :, :, :, 0 : {3: LANE, 4: WIDE, 5: HALF}[phase]]

    def arrived(phase, c):
        if phase == 0:
            wait_bytes(w_total(1, c), r0.at[c])
        else:
            wait_bytes(w_total(phase, c), pr.at[phase - 1, c])
            wait_bytes(w_total(phase, c), ps.at[phase - 1, c])

    def advance(phase, c):
        arrived(phase - 1, c)
        for ref, to in parts(phase, c):
            remote(ref, ref, ps.at[phase - 1, c], pr.at[phase - 1, c], to).start()

    def fwd_tile(c, i):
        at = slice(i * tile, i * tile + tile)
        x32 = h[c % H_SLOTS, at, :].astype(F32)
        inv = lax.rsqrt(jnp.mean(x32 * x32, axis=-1, keepdims=True) + NORM_EPS)
        n = (x32 * inv).astype(BF16)
        acc = x32
        ahead = mat(n, square(w, c, 0, 0)), mat(n, square(w, c, 1, 0))
        for k in range(4):
            a, b = ahead
            if k < 3:
                ahead = mat(n, square(w, c, 0, k + 1)), mat(n, square(w, c, 1, k + 1))
            u = (a * jax.nn.sigmoid(a) * b).astype(BF16)
            acc += mat(u, out_square(w, c, k))
        h[(c + 1) % H_SLOTS, at, :] = acc.astype(BF16)

    def keep(c):
        return pltpu.make_async_copy(h.at[c % H_SLOTS], h_all.at[c], hsem.at[c])

    def recall(c):
        return pltpu.make_async_copy(h_all.at[c], h.at[c % H_SLOTS], hsem.at[c])

    n_kept = n_block - H_SLOTS
    lead = (max(P_AHEAD) + TICKS - 1) // TICKS

    def gather(j, r):
        for k in (5, 4, 3, 2, 1):
            if (P_AHEAD[k] + r) % TICKS == 0:
                c = j + (P_AHEAD[k] + r) // TICKS

                @pl.when((c >= 0) & (c < n_block))
                def _(k=k, c=c):
                    advance(k, c)

    def lead_step(i, carry):
        for r in range(TICKS):
            gather(i - lead, r)
        return carry

    def fwd_step(c, carry):
        for r in range(TICKS):
            gather(c, r)
            if r == 0:
                arrived(5, c)

                @pl.when((c >= 2) & (c - 2 < n_kept))
                def _():
                    keep(c - 2).wait()

            if r == 1:

                @pl.when(c < n_kept)
                def _():
                    keep(c).start()

            fwd_tile(c, r)
        return carry

    lax.fori_loop(0, lead, lead_step, 0)
    load_h.wait()
    lax.fori_loop(0, n_block - 1, fwd_step, 0)
    arrived(5, n_block - 1)
    load_e.wait()

    def g_total(phase):
        if phase == 1:
            return x1.at[0]
        if phase == 2:
            return x1.at[0, :, :, :, :, 0:WIDE]
        if phase == 3:
            return x1.at[0, :, :, :, :, 0:LANE]
        if phase == 4:
            return x1.at[0, :, :, 0, :, 0:LANE]
        return x1.at[0, :, 0, 0, :, 0:LANE]

    def slot_of(phase, b):
        return b % Q_SLOTS[phase]

    def push(phase, b, moves):
        slot = slot_of(phase, b)
        for src, dst, to in moves:
            remote(src, dst, qs.at[phase - 1, slot], qr.at[phase - 1, slot], to).start()

    def taken(phase, b):
        slot = slot_of(phase, b)
        wait_bytes(g_total(phase), qr.at[phase - 1, slot])
        wait_bytes(g_total(phase), qs.at[phase - 1, slot])

    def q1(b):
        push(1, b, ((g.at[b % 2, :, :, :, :, col(HALF - HALF * core, HALF)], x1.at[slot_of(1, b)], here.to_core),))

    def q2(b):
        taken(1, b)
        q, t, p = slot_of(1, b), slot_of(2, b), b % 2
        for m in range(3):
            for f in range(2):
                for k in range(2):
                    x1[q, m, f, k] += g[p, m, f, k, :, col(HALF * core, HALF)]
        push(2, b, (
            (x1.at[q, 0, :, :, :, col(WIDE - WIDE * x, WIDE)], x2g.at[t], here.to_x),
            (x1.at[q, 1, :, :, :, col(WIDE - WIDE * y, WIDE)], x2i.at[t], here.to_y),
            (x1.at[q, 2, :, 1 - zn], x2o.at[t], here.to_zn),
        ))

    def q3(b):
        taken(2, b)
        o, q, t = slot_of(1, b), slot_of(2, b), slot_of(3, b)
        for f in range(2):
            for k in range(2):
                x2g[q, f, k] += x1[o, 0, f, k, :, col(WIDE * x, WIDE)]
                x2i[q, f, k] += x1[o, 1, f, k, :, col(WIDE * y, WIDE)]
            x2o[q, f] += x1[o, 2, f, zn]
        push(3, b, (
            (x2g.at[q, :, :, LO, col(LANE - LANE * y, LANE)], x3gl.at[t], here.to_y),
            (x2i.at[q, :, :, LO, col(LANE - LANE * x, LANE)], x3il.at[t], here.to_x),
            (x2g.at[q, :, 1 - zn, HI], x3gh.at[t], here.to_zn),
            (x2i.at[q, :, 1 - zn, HI], x3ih.at[t], here.to_zn),
            (x2o.at[q, :, LO, col(WIDE - WIDE * x, WIDE)], x3a.at[t], here.to_x),
            (x2o.at[q, :, HI, col(WIDE - WIDE * y, WIDE)], x3b.at[t], here.to_y),
        ))

    def q4(b):
        taken(3, b)
        o, q, t = slot_of(2, b), slot_of(3, b), slot_of(4, b)
        for f in range(2):
            for k in range(2):
                x3gl[q, f, k] += x2g[o, f, k, LO, col(LANE * y, LANE)]
                x3il[q, f, k] += x2i[o, f, k, LO, col(LANE * x, LANE)]
            x3gh[q, f] += x2g[o, f, zn, HI]
            x3ih[q, f] += x2i[o, f, zn, HI]
            x3a[q, f] += x2o[o, f, LO, col(WIDE * x, WIDE)]
            x3b[q, f] += x2o[o, f, HI, col(WIDE * y, WIDE)]
        push(4, b, (
            (x3gl.at[q, :, 1 - zn], x4g.at[t, :, LO], here.to_zn),
            (x3il.at[q, :, 1 - zn], x4i.at[t, :, LO], here.to_zn),
            (x3gh.at[q, :, :, col(LANE - LANE * y, LANE)], x4g.at[t, :, HI], here.to_y),
            (x3ih.at[q, :, :, col(LANE - LANE * x, LANE)], x4i.at[t, :, HI], here.to_x),
            (x3a.at[q, :, :, col(LANE - LANE * y, LANE)], x4a.at[t], here.to_y),
            (x3b.at[q, :, :, col(LANE - LANE * x, LANE)], x4b.at[t], here.to_x),
        ))

    def q5(b):
        taken(4, b)
        o, q, t = slot_of(3, b), slot_of(4, b), slot_of(5, b)
        for f in range(2):
            x4g[q, f, LO] += x3gl[o, f, zn]
            x4i[q, f, LO] += x3il[o, f, zn]
            x4g[q, f, HI] += x3gh[o, f, :, col(LANE * y, LANE)]
            x4i[q, f, HI] += x3ih[o, f, :, col(LANE * x, LANE)]
            x4a[q, f] += x3a[o, f, :, col(LANE * y, LANE)]
            x4b[q, f] += x3b[o, f, :, col(LANE * x, LANE)]
        push(5, b, (
            (x4g.at[q, 1 - zf], x5g.at[t], here.to_zf),
            (x4i.at[q, 1 - zf], x5i.at[t], here.to_zf),
            (x4a.at[q, 1 - zf], x5a.at[t], here.to_zf),
            (x4b.at[q, 1 - zf], x5b.at[t], here.to_zf),
        ))

    def q6(b):
        taken(5, b)
        o, q = slot_of(4, b), slot_of(5, b)
        c = n_block - 1 - b
        v, p = c // n_stage, c % n_stage
        t = b % F_SLOTS

        @pl.when(b >= F_SLOTS)
        def _():
            wait_bytes(g_total(5), own.at[t])

        fg[t] = x5g[q] + x4g[o, zf]
        fi[t] = x5i[q] + x4i[o, zf]
        fa[t] = x5a[q] + x4a[o, zf]
        fb[t] = x5b[q] + x4b[o, zf]
        moves = (
            (fg.at[t], gg.at[v, 0, :, col(c_g, LANE)]),
            (fi.at[t], gi.at[v, 0, :, col(c_i, LANE)]),
            (fa.at[t], go.at[v, 0, pl.ds(pl.multiple_of(PIECE * (2 * core + x), SUB), SUB), col(LANE * y, LANE)]),
            (fb.at[t], go.at[v, 0, pl.ds(pl.multiple_of(PIECE * (2 * core + y) + SUB, SUB), SUB), col(LANE * x, LANE)]),
        )

        @pl.when(p == s)
        def _():
            for src, dst in moves:
                pltpu.make_async_copy(src, dst, own.at[t]).start()

        @pl.when(p != s)
        def _():
            for src, dst in moves:
                remote(src, dst, own.at[t], fsem.at[v], (z, p)).start()

    def bwd_tile(b, i):
        at = slice(i * tile, i * tile + tile)
        p, c = b % 2, n_block - 1 - b
        x32 = h[c % H_SLOTS, at, :].astype(F32)
        inv = lax.rsqrt(jnp.mean(x32 * x32, axis=-1, keepdims=True) + NORM_EPS)
        hr = x32 * inv
        n = hr.astype(BF16)
        et = e[0, at, :]
        q = jnp.zeros((tile, WIDE), F32)

        def add(m, k, value):
            for f in range(2):
                for r in range(2):
                    part = value[LANE * f + PIECE * r : LANE * f + PIECE * r + PIECE]
                    if i > 0:
                        part += g[p, m, f, r, :, WIDE * k : WIDE * k + WIDE]
                    g[p, m, f, r, :, WIDE * k : WIDE * k + WIDE] = part

        def up(k):
            return mat(n, square(w, c, 0, k)), mat(n, square(w, c, 1, k)), mat_cols(et, out_square(w, c, k))

        ahead = up(0)
        for k in range(4):
            a, bb, t = ahead
            if k < 3:
                ahead = up(k + 1)
            sg = jax.nn.sigmoid(a)
            act = a * sg
            u = (act * bb).astype(BF16)
            da = (t * bb * sg * (1.0 + a * (1.0 - sg))).astype(BF16)
            db = (t * act).astype(BF16)
            q += mat_cols(da, square(w, c, 0, k)) + mat_cols(db, square(w, c, 1, k))
            add(0, k, mat_rows(n, da))
            add(1, k, mat_rows(n, db))
            do = mat_rows(u, et)
            for j in range(4):
                part = do[PIECE * j : PIECE * j + PIECE]
                if i > 0:
                    part += g[p, 2, k // 2, k % 2, :, WIDE * j : WIDE * j + WIDE]
                g[p, 2, k // 2, k % 2, :, WIDE * j : WIDE * j + WIDE] = part
        grad = et.astype(F32) + inv * (q - hr * jnp.mean(q * hr, axis=-1, keepdims=True))
        e[0, at, :] = grad.astype(BF16)

    def scatter_sums(j, r):
        for k, fn in ((1, q1), (6, q6), (5, q5), (4, q4), (3, q3), (2, q2)):
            if Q_AT[k] % TICKS == r:
                b = j - Q_AT[k] // TICKS

                @pl.when((b >= 0) & (b < n_block))
                def _(fn=fn, b=b):
                    fn(b)

    def drain_step(j, carry):
        for r in range(TICKS):
            scatter_sums(j, r)
        return carry

    def bwd_step(b, carry):
        c = n_block - 1 - b
        for r in range(TICKS):
            scatter_sums(b, r)
            if r == 0:

                @pl.when(c < n_kept)
                def _():
                    recall(c).wait()

                @pl.when((c - 2 >= 0) & (c - 2 < n_kept))
                def _():
                    recall(c - 2).start()

            bwd_tile(b, r)
        return carry

    half = rows // 2
    lo, hi = pl.ds(0, half), pl.ds(half, half)

    def share(k, src, dst, part, to):
        return remote(e.at[src, part], e.at[dst, part], as_.at[k], ar.at[k], to)

    shares = (
        share(0, 0, 1, lo, here.to_x),
        share(1, 0, 2, lo, here.to_y),
        share(2, 0, 2, hi, here.to_y),
        share(3, 0, 1, hi, here.to_x),
        share(4, 1, 3, lo, here.to_y),
        share(5, 2, 3, hi, here.to_x),
    )
    needs = {4: 0, 5: 2}
    own_slots = (s, here.to_x[1], here.to_y[1], 2 * (n_stage // 2 - 1 - s // 2) + core)
    hands = []
    for k, slot in enumerate(own_slots):
        hands.append(remote(e.at[k], ga.at[slot], cs.at[k], cr.at[k], here.to_core))
        hands.append(pltpu.make_async_copy(e.at[k], ga.at[slot], cl.at[k]))

    def hand(k):
        for copy in hands[2 * k : 2 * k + 2]:
            copy.start()

    lax.fori_loop(0, n_block, bwd_step, 0)
    for copy in shares[:4]:
        copy.start()
    hand(0)
    lax.fori_loop(n_block, n_block + RELAY_AT, drain_step, 0)
    for k in needs:
        shares[needs[k]].wait_recv()
        shares[k].start()
    lax.fori_loop(n_block + RELAY_AT, n_block + HAND_AT, drain_step, 0)
    shares[3].wait_recv()
    hand(1)
    shares[1].wait_recv()
    hand(2)
    lax.fori_loop(n_block + HAND_AT, n_block + max(Q_AT) // TICKS + 1, drain_step, 0)
    shares[4].wait_recv()
    shares[5].wait_recv()
    hand(3)
    for copy in shares:
        copy.wait_send()

    def finish(t, carry):
        wait_bytes(g_total(5), own.at[t])
        return carry

    lax.fori_loop(0, F_SLOTS, finish, 0)
    for v in range(n_v):
        wait_bytes(w.at[0, :, 0, 0, :, 0 : LANE * (n_stage - 1)], s0.at[v])
        wait_bytes(g.at[0, :, 0, 0, :, 0 : LANE * (n_stage - 1)], fsem.at[v])
    for copy in hands:
        copy.wait()


def settle_kernel(*refs):
    n = (len(refs) - 2) // 3
    srcs, dsts, bufs, (rsem, wsem) = refs[:n], refs[n : 2 * n], refs[2 * n : 3 * n], refs[3 * n :]
    moves = []
    for a in range(n):
        for i in range(srcs[a].shape[0]):
            k = len(moves)
            moves.append((
                pltpu.make_async_copy(srcs[a].at[i], bufs[a].at[i], rsem.at[k]),
                pltpu.make_async_copy(bufs[a].at[i], dsts[a].at[i], wsem.at[k]),
            ))
    for read, _ in moves:
        read.start()
    for read, write in moves:
        read.wait()
        write.start()
    for _, write in moves:
        write.wait()


def solution(mesh):
    n_stage = mesh.shape["stage"]
    act_spec = P(None, "data", None, None)
    w_spec = P(None, "stage", "data", None)
    hbm = pl.BlockSpec(memory_space=pltpu.HBM)
    dma = pltpu.SemaphoreType.DMA

    def body(act_in, cot_out, w_gate, w_in, w_out):
        n_micro, n_seq, n_tok, width = act_in.shape
        n_v, _, _, ffn = w_gate.shape
        n_block = n_v * n_stage
        rows = n_micro // n_stage * n_seq * n_tok
        block = (3, 2, 2, PIECE, ffn)
        flops = 2 * rows * width * ffn * n_block

        def f32(*shape):
            return pltpu.VMEM(shape, F32)

        def bf16(*shape):
            return pltpu.VMEM(shape, BF16)

        _, n1, n2, n3, n4, n5 = Q_SLOTS
        results = (
            jax.ShapeDtypeStruct(w_gate.shape, F32),
            jax.ShapeDtypeStruct(w_in.shape, F32),
            jax.ShapeDtypeStruct(w_out.shape, F32),
            jax.ShapeDtypeStruct((n_stage, rows, width), BF16),
        )
        *done, _ = pl.pallas_call(
            functools.partial(step_kernel, n_stage),
            name="step",
            out_shape=(*results, jax.ShapeDtypeStruct((n_block - H_SLOTS, rows, width), BF16)),
            in_specs=[hbm] * 5,
            out_specs=[hbm] * 5,
            scratch_shapes=[
                bf16(n_block, *block),
                bf16(H_SLOTS, rows, width),
                bf16(4, rows, width),
                f32(2, *block),
                f32(n1, 3, 2, 2, PIECE, HALF),
                f32(n2, 2, 2, PIECE, WIDE),
                f32(n2, 2, 2, PIECE, WIDE),
                f32(n2, 2, PIECE, HALF),
                f32(n3, 2, 2, SUB, LANE),
                f32(n3, 2, 2, SUB, LANE),
                f32(n3, 2, SUB, WIDE),
                f32(n3, 2, SUB, WIDE),
                f32(n3, 2, SUB, WIDE),
                f32(n3, 2, SUB, WIDE),
                f32(n4, 2, PIECE, LANE),
                f32(n4, 2, PIECE, LANE),
                f32(n4, 2, SUB, LANE),
                f32(n4, 2, SUB, LANE),
                f32(n5, PIECE, LANE),
                f32(n5, PIECE, LANE),
                f32(n5, SUB, LANE),
                f32(n5, SUB, LANE),
                f32(F_SLOTS, PIECE, LANE),
                f32(F_SLOTS, PIECE, LANE),
                f32(F_SLOTS, SUB, LANE),
                f32(F_SLOTS, SUB, LANE),
                dma((n_v,)),
                dma((n_block,)),
                dma((5, n_block)),
                dma((5, n_block)),
                dma((5, max(Q_SLOTS))),
                dma((5, max(Q_SLOTS))),
                dma((F_SLOTS,)),
                dma((n_v,)),
                dma((n_block,)),
                dma((2,)),
                dma((6,)),
                dma((6,)),
                dma((4,)),
                dma((4,)),
                dma((4,)),
            ],
            compiler_params=pltpu.CompilerParams(collective_id=0, has_side_effects=True, vmem_limit_bytes=67_000_000),
            cost_estimate=pl.CostEstimate(flops=11 * flops, bytes_accessed=2**26, transcendentals=0),
        )(act_in.reshape(n_stage, rows, width), cot_out.reshape(n_stage, rows, width), w_gate, w_in, w_out)
        moved = sum(a.shape[0] for a in done)
        gg, gi, go, ga = pl.pallas_call(
            settle_kernel,
            name="settle",
            out_shape=results,
            in_specs=[hbm] * 4,
            out_specs=[hbm] * 4,
            scratch_shapes=[pltpu.VMEM(a.shape, a.dtype) for a in done] + [dma((moved,)), dma((moved,))],
        )(*done)
        return ga.reshape(act_in.shape), gg, gi, go

    return jax.shard_map(body, mesh=mesh, in_specs=(act_spec, act_spec, w_spec, w_spec, w_spec), out_specs=(act_spec, w_spec, w_spec, w_spec), check_vma=False)
```

```python
import functools

import jax
import jax.numpy as jnp
from jax import lax
from jax.experimental import pallas as pl
from jax.experimental.pallas import tpu as pltpu
from jax.sharding import PartitionSpec as P

NORM_EPS = 1e-6
MESH = pl.DeviceIdType.MESH
TICKS = 3
H_SLOTS = 3
F_SLOTS = 6
P_AHEAD = (0, 20, 15, 11, 5, 2)
Q_SLOTS = (0, 4, 7, 9, 9, 8)
Q_AT = (0, 3, 5, 10, 19, 27, 37)
RELAY_AT = 7
HAND_AT = 10
LANE, WIDE, HALF = 128, 256, 512
PIECE, SUB = 64, 32
LO, HI = slice(0, SUB), slice(SUB, PIECE)
MOST, REST = slice(0, 48), slice(48, PIECE)
F32 = jnp.float32
BF16 = jnp.bfloat16


class Place:
    def __init__(self):
        self.z, self.s = lax.axis_index("data"), lax.axis_index("stage")
        self.core, self.x, self.y = self.s % 2, (self.s // 2) % 2, self.s // 4
        self.zn, self.zf = self.z % 2, self.z // 2
        self.to_x = (self.z, self.s + 2 - 4 * self.x)
        self.to_y = (self.z, self.s + 4 - 8 * self.y)
        self.to_core = (self.z, self.s + 1 - 2 * self.core)
        self.to_zn = (self.z + 1 - 2 * self.zn, self.s)
        self.to_zf = (self.z + 2 - 4 * self.zf, self.s)


def col(start, size):
    return pl.ds(pl.multiple_of(start, LANE), size)


def narrow(core, hi, lo):
    return HALF * core + WIDE * hi + LANE * lo


def remote(src, dst, ssem, rsem, to):
    return pltpu.make_async_remote_copy(src_ref=src, dst_ref=dst, send_sem=ssem, recv_sem=rsem, device_id=to, device_id_type=MESH)


def wait_bytes(ref, sem):
    pltpu.make_async_copy(ref, ref, sem).wait()


def enter(here, n_stage):
    barrier = pltpu.get_barrier_semaphore()
    peers = [(here.z, (here.s + k) % n_stage) for k in range(1, n_stage)] + [here.to_zn, here.to_zf]
    for peer in peers:
        pl.semaphore_signal(barrier, inc=1, device_id=peer, device_id_type=MESH)
    pl.semaphore_wait(barrier, len(peers))


def mat_rows(left, right):
    return lax.dot_general(left, right, (((0,), (0,)), ((), ())), preferred_element_type=F32)


def mat_cols(left, right):
    return lax.dot_general(left, right, (((1,), (1,)), ((), ())), preferred_element_type=F32)


def mat(left, right):
    return jnp.dot(left, right, preferred_element_type=F32)


def square(w_ref, at, m, k):
    return w_ref[at, m, :, :, :, WIDE * k : WIDE * k + WIDE].reshape(WIDE, WIDE)


def out_square(w_ref, at, k):
    return jnp.concatenate([w_ref[at, 2, k // 2, k % 2, :, WIDE * j : WIDE * j + WIDE] for j in range(4)], axis=0)


def step_kernel(n_stage, act, cot, wg, wi, wo, gg, gi, go, ga, h_all, w, h, e, g, x1, x2g, x2i, x2o, x3gl, x3il, x3gh, x3ih, x3a, x3b, x4g, x4i, x4a, x4b, x5g, x5i, x5a, x5b, fg, fi, fa, fb, s0, r0, ps, pr, qs, qr, own, fsem, hsem, esem, as_, ar, cs, cr, cl):
    here = Place()
    z, s, zn, zf, x, y, core = here.z, here.s, here.zn, here.zf, here.x, here.y, here.core
    n_block = w.shape[0]
    n_v = n_block // n_stage
    rows = h.shape[1]
    tile = rows // TICKS
    c_g, c_i = narrow(core, x, y), narrow(core, y, x)
    c_x, c_y, c_c = narrow(core, x, 0), narrow(core, y, 0), narrow(core, 0, 0)

    enter(here, n_stage)
    load_h = pltpu.make_async_copy(act.at[s], h.at[0], esem.at[0])
    load_e = pltpu.make_async_copy(cot.at[s], e.at[0], esem.at[1])
    load_h.start()

    def scatter(v, k):
        q = (s + k) % n_stage
        core, x, y = q % 2, (q // 2) % 2, q // 4
        d_g, d_i = narrow(core, x, y), narrow(core, y, x)
        c = v * n_stage + s
        moves = (
            (wg.at[v, 0, :, col(d_g, LANE)], w.at[c, 0, zf, zn, :, col(d_g, LANE)]),
            (wi.at[v, 0, :, col(d_i, LANE)], w.at[c, 1, zf, zn, :, col(d_i, LANE)]),
            (wo.at[v, 0, pl.ds(pl.multiple_of(PIECE * (2 * core + x), SUB), SUB), col(LANE * y, LANE)], w.at[c, 2, zf, zn, 0:SUB, col(d_g, LANE)]),
            (wo.at[v, 0, pl.ds(pl.multiple_of(PIECE * (2 * core + y) + SUB, SUB), SUB), col(LANE * x, LANE)], w.at[c, 2, zf, zn, SUB:PIECE, col(d_i, LANE)]),
        )
        for src, dst in moves:
            if k == 0:
                pltpu.make_async_copy(src, dst, r0.at[c]).start()
            else:
                remote(src, dst, s0.at[v], r0.at[c], (z, q)).start()

    for v in range(n_v):
        for k in range(n_stage):
            scatter(v, k)
    load_e.start()

    def parts(phase, c):
        if phase == 1:
            return (
                (w.at[c, 0, zf, zn, :, col(c_g, LANE)], here.to_zf),
                (w.at[c, 1, zf, zn, :, col(c_i, LANE)], here.to_zf),
                (w.at[c, 2, zf, zn, 0:SUB, col(c_g, LANE)], here.to_zf),
                (w.at[c, 2, zf, zn, SUB:PIECE, col(c_i, LANE)], here.to_zf),
            )
        if phase == 2:
            return (
                (w.at[c, 0, :, zn, MOST, col(c_g, LANE)], here.to_zn),
                (w.at[c, 0, :, zn, REST, col(c_g, LANE)], here.to_y),
                (w.at[c, 1, :, zn, MOST, col(c_i, LANE)], here.to_zn),
                (w.at[c, 1, :, zn, REST, col(c_i, LANE)], here.to_x),
                (w.at[c, 2, :, zn, 0:SUB, col(c_g, LANE)], here.to_y),
                (w.at[c, 2, :, zn, SUB:PIECE, col(c_i, LANE)], here.to_x),
            )
        if phase == 3:
            return (
                (w.at[c, 0, :, :, MOST, col(c_g, LANE)], here.to_y),
                (w.at[c, 0, :, zn, REST, col(c_x, WIDE)], here.to_zn),
                (w.at[c, 1, :, :, MOST, col(c_i, LANE)], here.to_x),
                (w.at[c, 1, :, zn, REST, col(c_y, WIDE)], here.to_zn),
                (w.at[c, 2, :, zn, 0:SUB, col(c_x, WIDE)], here.to_x),
                (w.at[c, 2, :, zn, SUB:PIECE, col(c_y, WIDE)], here.to_y),
            )
        if phase == 4:
            return (
                (w.at[c, 0, :, :, :, col(c_x, WIDE)], here.to_x),
                (w.at[c, 1, :, :, :, col(c_y, WIDE)], here.to_y),
                (w.at[c, 2, :, zn, :, col(c_c, HALF)], here.to_zn),
            )
        return ((w.at[c, :, :, :, :, col(c_c, HALF)], here.to_core),)

    def w_total(phase, c):
        if phase == 1:
            return w.at[c, :, 0, 0, :, 0:LANE]
        if phase == 2:
            return w.at[c, :, :, 0, :, 0:LANE]
        return w.at[c, :, :, :, :, 0 : {3: LANE, 4: WIDE, 5: HALF}[phase]]

    def arrived(phase, c):
        if phase == 0:
            wait_bytes(w_total(1, c), r0.at[c])
        else:
            wait_bytes(w_total(phase, c), pr.at[phase - 1, c])
            wait_bytes(w_total(phase, c), ps.at[phase - 1, c])

    def advance(phase, c):
        arrived(phase - 1, c)
        for ref, to in parts(phase, c):
            remote(ref, ref, ps.at[phase - 1, c], pr.at[phase - 1, c], to).start()

    def fwd_tile(c, i):
        at = slice(i * tile, i * tile + tile)
        x32 = h[c % H_SLOTS, at, :].astype(F32)
        inv = lax.rsqrt(jnp.mean(x32 * x32, axis=-1, keepdims=True) + NORM_EPS)
        n = (x32 * inv).astype(BF16)
        acc = x32
        ahead = mat(n, square(w, c, 0, 0)), mat(n, square(w, c, 1, 0))
        for k in range(4):
            a, b = ahead
            if k < 3:
                ahead = mat(n, square(w, c, 0, k + 1)), mat(n, square(w, c, 1, k + 1))
            u = (a * jax.nn.sigmoid(a) * b).astype(BF16)
            acc += mat(u, out_square(w, c, k))
        h[(c + 1) % H_SLOTS, at, :] = acc.astype(BF16)

    def keep(c):
        return pltpu.make_async_copy(h.at[c % H_SLOTS], h_all.at[c], hsem.at[c])

    def recall(c):
        return pltpu.make_async_copy(h_all.at[c], h.at[c % H_SLOTS], hsem.at[c])

    n_kept = n_block - H_SLOTS
    lead = (max(P_AHEAD) + TICKS - 1) // TICKS

    def gather(j, r):
        for k in (5, 4, 3, 2, 1):
            if (P_AHEAD[k] + r) % TICKS == 0:
                c = j + (P_AHEAD[k] + r) // TICKS

                @pl.when((c >= 0) & (c < n_block))
                def _(k=k, c=c):
                    advance(k, c)

    def lead_step(i, carry):
        for r in range(TICKS):
            gather(i - lead, r)
        return carry

    def fwd_step(c, carry):
        for r in range(TICKS):
            gather(c, r)
            if r == 0:
                arrived(5, c)

                @pl.when((c >= 2) & (c - 2 < n_kept))
                def _():
                    keep(c - 2).wait()

            if r == 1:

                @pl.when(c < n_kept)
                def _():
                    keep(c).start()

            fwd_tile(c, r)
        return carry

    lax.fori_loop(0, lead, lead_step, 0)
    load_h.wait()
    lax.fori_loop(0, n_block - 1, fwd_step, 0)
    arrived(5, n_block - 1)
    load_e.wait()

    def g_total(phase):
        if phase == 1:
            return x1.at[0]
        if phase == 2:
            return x1.at[0, :, :, :, :, 0:WIDE]
        if phase == 3:
            return x1.at[0, :, :, :, :, 0:LANE]
        if phase == 4:
            return x1.at[0, :, :, 0, :, 0:LANE]
        return x1.at[0, :, 0, 0, :, 0:LANE]

    def slot_of(phase, b):
        return b % Q_SLOTS[phase]

    def push(phase, b, moves):
        slot = slot_of(phase, b)
        for src, dst, to in moves:
            remote(src, dst, qs.at[phase - 1, slot], qr.at[phase - 1, slot], to).start()

    def taken(phase, b):
        slot = slot_of(phase, b)
        wait_bytes(g_total(phase), qr.at[phase - 1, slot])
        wait_bytes(g_total(phase), qs.at[phase - 1, slot])

    def q1(b):
        push(1, b, ((g.at[b % 2, :, :, :, :, col(HALF - HALF * core, HALF)], x1.at[slot_of(1, b)], here.to_core),))

    def q2(b):
        taken(1, b)
        q, t, p = slot_of(1, b), slot_of(2, b), b % 2
        for m in range(3):
            for f in range(2):
                for k in range(2):
                    x1[q, m, f, k] += g[p, m, f, k, :, col(HALF * core, HALF)]
        push(2, b, (
            (x1.at[q, 0, :, :, :, col(WIDE - WIDE * x, WIDE)], x2g.at[t], here.to_x),
            (x1.at[q, 1, :, :, :, col(WIDE - WIDE * y, WIDE)], x2i.at[t], here.to_y),
            (x1.at[q, 2, :, 1 - zn], x2o.at[t], here.to_zn),
        ))

    def q3(b):
        taken(2, b)
        o, q, t = slot_of(1, b), slot_of(2, b), slot_of(3, b)
        for f in range(2):
            for k in range(2):
                x2g[q, f, k] += x1[o, 0, f, k, :, col(WIDE * x, WIDE)]
                x2i[q, f, k] += x1[o, 1, f, k, :, col(WIDE * y, WIDE)]
            x2o[q, f] += x1[o, 2, f, zn]
        push(3, b, (
            (x2g.at[q, :, :, LO, col(LANE - LANE * y, LANE)], x3gl.at[t], here.to_y),
            (x2i.at[q, :, :, LO, col(LANE - LANE * x, LANE)], x3il.at[t], here.to_x),
            (x2g.at[q, :, 1 - zn, HI], x3gh.at[t], here.to_zn),
            (x2i.at[q, :, 1 - zn, HI], x3ih.at[t], here.to_zn),
            (x2o.at[q, :, LO, col(WIDE - WIDE * x, WIDE)], x3a.at[t], here.to_x),
            (x2o.at[q, :, HI, col(WIDE - WIDE * y, WIDE)], x3b.at[t], here.to_y),
        ))

    def q4(b):
        taken(3, b)
        o, q, t = slot_of(2, b), slot_of(3, b), slot_of(4, b)
        for f in range(2):
            for k in range(2):
                x3gl[q, f, k] += x2g[o, f, k, LO, col(LANE * y, LANE)]
                x3il[q, f, k] += x2i[o, f, k, LO, col(LANE * x, LANE)]
            x3gh[q, f] += x2g[o, f, zn, HI]
            x3ih[q, f] += x2i[o, f, zn, HI]
            x3a[q, f] += x2o[o, f, LO, col(WIDE * x, WIDE)]
            x3b[q, f] += x2o[o, f, HI, col(WIDE * y, WIDE)]
        push(4, b, (
            (x3gl.at[q, :, 1 - zn], x4g.at[t, :, LO], here.to_zn),
            (x3il.at[q, :, 1 - zn], x4i.at[t, :, LO], here.to_zn),
            (x3gh.at[q, :, :, col(LANE - LANE * y, LANE)], x4g.at[t, :, HI], here.to_y),
            (x3ih.at[q, :, :, col(LANE - LANE * x, LANE)], x4i.at[t, :, HI], here.to_x),
            (x3a.at[q, :, :, col(LANE - LANE * y, LANE)], x4a.at[t], here.to_y),
            (x3b.at[q, :, :, col(LANE - LANE * x, LANE)], x4b.at[t], here.to_x),
        ))

    def q5(b):
        taken(4, b)
        o, q, t = slot_of(3, b), slot_of(4, b), slot_of(5, b)
        for f in range(2):
            x4g[q, f, LO] += x3gl[o, f, zn]
            x4i[q, f, LO] += x3il[o, f, zn]
            x4g[q, f, HI] += x3gh[o, f, :, col(LANE * y, LANE)]
            x4i[q, f, HI] += x3ih[o, f, :, col(LANE * x, LANE)]
            x4a[q, f] += x3a[o, f, :, col(LANE * y, LANE)]
            x4b[q, f] += x3b[o, f, :, col(LANE * x, LANE)]
        push(5, b, (
            (x4g.at[q, 1 - zf], x5g.at[t], here.to_zf),
            (x4i.at[q, 1 - zf], x5i.at[t], here.to_zf),
            (x4a.at[q, 1 - zf], x5a.at[t], here.to_zf),
            (x4b.at[q, 1 - zf], x5b.at[t], here.to_zf),
        ))

    def q6(b):
        taken(5, b)
        o, q = slot_of(4, b), slot_of(5, b)
        c = n_block - 1 - b
        v, p = c // n_stage, c % n_stage
        t = b % F_SLOTS

        @pl.when(b >= F_SLOTS)
        def _():
            wait_bytes(g_total(5), own.at[t])

        fg[t] = x5g[q] + x4g[o, zf]
        fi[t] = x5i[q] + x4i[o, zf]
        fa[t] = x5a[q] + x4a[o, zf]
        fb[t] = x5b[q] + x4b[o, zf]
        moves = (
            (fg.at[t], gg.at[v, 0, :, col(c_g, LANE)]),
            (fi.at[t], gi.at[v, 0, :, col(c_i, LANE)]),
            (fa.at[t], go.at[v, 0, pl.ds(pl.multiple_of(PIECE * (2 * core + x), SUB), SUB), col(LANE * y, LANE)]),
            (fb.at[t], go.at[v, 0, pl.ds(pl.multiple_of(PIECE * (2 * core + y) + SUB, SUB), SUB), col(LANE * x, LANE)]),
        )

        @pl.when(p == s)
        def _():
            for src, dst in moves:
                pltpu.make_async_copy(src, dst, own.at[t]).start()

        @pl.when(p != s)
        def _():
            for src, dst in moves:
                remote(src, dst, own.at[t], fsem.at[v], (z, p)).start()

    def bwd_tile(b, i):
        at = slice(i * tile, i * tile + tile)
        p, c = b % 2, n_block - 1 - b
        x32 = h[c % H_SLOTS, at, :].astype(F32)
        inv = lax.rsqrt(jnp.mean(x32 * x32, axis=-1, keepdims=True) + NORM_EPS)
        hr = x32 * inv
        n = hr.astype(BF16)
        et = e[0, at, :]
        q = jnp.zeros((tile, WIDE), F32)

        def add(m, k, value):
            for f in range(2):
                for r in range(2):
                    part = value[LANE * f + PIECE * r : LANE * f + PIECE * r + PIECE]
                    if i > 0:
                        part += g[p, m, f, r, :, WIDE * k : WIDE * k + WIDE]
                    g[p, m, f, r, :, WIDE * k : WIDE * k + WIDE] = part

        def up(k):
            return mat(n, square(w, c, 0, k)), mat(n, square(w, c, 1, k)), mat_cols(et, out_square(w, c, k))

        ahead = up(0)
        for k in range(4):
            a, bb, t = ahead
            if k < 3:
                ahead = up(k + 1)
            sg = jax.nn.sigmoid(a)
            act = a * sg
            u = (act * bb).astype(BF16)
            da = (t * bb * sg * (1.0 + a * (1.0 - sg))).astype(BF16)
            db = (t * act).astype(BF16)
            q += mat_cols(da, square(w, c, 0, k)) + mat_cols(db, square(w, c, 1, k))
            add(0, k, mat_rows(n, da))
            add(1, k, mat_rows(n, db))
            do = mat_rows(u, et)
            for j in range(4):
                part = do[PIECE * j : PIECE * j + PIECE]
                if i > 0:
                    part += g[p, 2, k // 2, k % 2, :, WIDE * j : WIDE * j + WIDE]
                g[p, 2, k // 2, k % 2, :, WIDE * j : WIDE * j + WIDE] = part
        grad = et.astype(F32) + inv * (q - hr * jnp.mean(q * hr, axis=-1, keepdims=True))
        e[0, at, :] = grad.astype(BF16)

    def scatter_sums(j, r):
        for k, fn in ((1, q1), (6, q6), (5, q5), (4, q4), (3, q3), (2, q2)):
            if Q_AT[k] % TICKS == r:
                b = j - Q_AT[k] // TICKS

                @pl.when((b >= 0) & (b < n_block))
                def _(fn=fn, b=b):
                    fn(b)

    def drain_step(j, carry):
        for r in range(TICKS):
            scatter_sums(j, r)
        return carry

    def bwd_step(b, carry):
        c = n_block - 1 - b
        for r in range(TICKS):
            scatter_sums(b, r)
            if r == 0:

                @pl.when(c < n_kept)
                def _():
                    recall(c).wait()

                @pl.when((c - 2 >= 0) & (c - 2 < n_kept))
                def _():
                    recall(c - 2).start()

            bwd_tile(b, r)
        return carry

    half = rows // 2
    lo, hi = pl.ds(0, half), pl.ds(half, half)

    def share(k, src, dst, part, to):
        return remote(e.at[src, part], e.at[dst, part], as_.at[k], ar.at[k], to)

    shares = (
        share(0, 0, 1, lo, here.to_x),
        share(1, 0, 2, lo, here.to_y),
        share(2, 0, 2, hi, here.to_y),
        share(3, 0, 1, hi, here.to_x),
        share(4, 1, 3, lo, here.to_y),
        share(5, 2, 3, hi, here.to_x),
    )
    needs = {4: 0, 5: 2}
    own_slots = (s, here.to_x[1], here.to_y[1], 2 * (n_stage // 2 - 1 - s // 2) + core)
    hands = []
    for k, slot in enumerate(own_slots):
        hands.append(remote(e.at[k], ga.at[slot], cs.at[k], cr.at[k], here.to_core))
        hands.append(pltpu.make_async_copy(e.at[k], ga.at[slot], cl.at[k]))

    def hand(k):
        for copy in hands[2 * k : 2 * k + 2]:
            copy.start()

    lax.fori_loop(0, n_block, bwd_step, 0)
    for copy in shares[:4]:
        copy.start()
    hand(0)
    lax.fori_loop(n_block, n_block + RELAY_AT, drain_step, 0)
    for k in needs:
        shares[needs[k]].wait_recv()
        shares[k].start()
    lax.fori_loop(n_block + RELAY_AT, n_block + HAND_AT, drain_step, 0)
    shares[3].wait_recv()
    hand(1)
    shares[1].wait_recv()
    hand(2)
    lax.fori_loop(n_block + HAND_AT, n_block + max(Q_AT) // TICKS + 1, drain_step, 0)
    shares[4].wait_recv()
    shares[5].wait_recv()
    hand(3)
    for copy in shares:
        copy.wait_send()

    def finish(t, carry):
        wait_bytes(g_total(5), own.at[t])
        return carry

    lax.fori_loop(0, F_SLOTS, finish, 0)
    for v in range(n_v):
        wait_bytes(w.at[0, :, 0, 0, :, 0 : LANE * (n_stage - 1)], s0.at[v])
        wait_bytes(g.at[0, :, 0, 0, :, 0 : LANE * (n_stage - 1)], fsem.at[v])
    for copy in hands:
        copy.wait()


def settle_kernel(*refs):
    n = (len(refs) - 2) // 3
    srcs, dsts, bufs, (rsem, wsem) = refs[:n], refs[n : 2 * n], refs[2 * n : 3 * n], refs[3 * n :]
    moves = []
    for a in range(n):
        for i in range(srcs[a].shape[0]):
            k = len(moves)
            moves.append((
                pltpu.make_async_copy(srcs[a].at[i], bufs[a].at[i], rsem.at[k]),
                pltpu.make_async_copy(bufs[a].at[i], dsts[a].at[i], wsem.at[k]),
            ))
    for read, _ in moves:
        read.start()
    for read, write in moves:
        read.wait()
        write.start()
    for _, write in moves:
        write.wait()


def solution(mesh):
    n_stage = mesh.shape["stage"]
    act_spec = P(None, "data", None, None)
    w_spec = P(None, "stage", "data", None)
    hbm = pl.BlockSpec(memory_space=pltpu.HBM)
    dma = pltpu.SemaphoreType.DMA

    def body(act_in, cot_out, w_gate, w_in, w_out):
        n_micro, n_seq, n_tok, width = act_in.shape
        n_v, _, _, ffn = w_gate.shape
        n_block = n_v * n_stage
        rows = n_micro // n_stage * n_seq * n_tok
        block = (3, 2, 2, PIECE, ffn)
        flops = 2 * rows * width * ffn * n_block

        def f32(*shape):
            return pltpu.VMEM(shape, F32)

        def bf16(*shape):
            return pltpu.VMEM(shape, BF16)

        _, n1, n2, n3, n4, n5 = Q_SLOTS
        results = (
            jax.ShapeDtypeStruct(w_gate.shape, F32),
            jax.ShapeDtypeStruct(w_in.shape, F32),
            jax.ShapeDtypeStruct(w_out.shape, F32),
            jax.ShapeDtypeStruct((n_stage, rows, width), BF16),
        )
        *done, _ = pl.pallas_call(
            functools.partial(step_kernel, n_stage),
            name="step",
            out_shape=(*results, jax.ShapeDtypeStruct((n_block - H_SLOTS, rows, width), BF16)),
            in_specs=[hbm] * 5,
            out_specs=[hbm] * 5,
            scratch_shapes=[
                bf16(n_block, *block),
                bf16(H_SLOTS, rows, width),
                bf16(4, rows, width),
                f32(2, *block),
                f32(n1, 3, 2, 2, PIECE, HALF),
                f32(n2, 2, 2, PIECE, WIDE),
                f32(n2, 2, 2, PIECE, WIDE),
                f32(n2, 2, PIECE, HALF),
                f32(n3, 2, 2, SUB, LANE),
                f32(n3, 2, 2, SUB, LANE),
                f32(n3, 2, SUB, WIDE),
                f32(n3, 2, SUB, WIDE),
                f32(n3, 2, SUB, WIDE),
                f32(n3, 2, SUB, WIDE),
                f32(n4, 2, PIECE, LANE),
                f32(n4, 2, PIECE, LANE),
                f32(n4, 2, SUB, LANE),
                f32(n4, 2, SUB, LANE),
                f32(n5, PIECE, LANE),
                f32(n5, PIECE, LANE),
                f32(n5, SUB, LANE),
                f32(n5, SUB, LANE),
                f32(F_SLOTS, PIECE, LANE),
                f32(F_SLOTS, PIECE, LANE),
                f32(F_SLOTS, SUB, LANE),
                f32(F_SLOTS, SUB, LANE),
                dma((n_v,)),
                dma((n_block,)),
                dma((5, n_block)),
                dma((5, n_block)),
                dma((5, max(Q_SLOTS))),
                dma((5, max(Q_SLOTS))),
                dma((F_SLOTS,)),
                dma((n_v,)),
                dma((n_block,)),
                dma((2,)),
                dma((6,)),
                dma((6,)),
                dma((4,)),
                dma((4,)),
                dma((4,)),
            ],
            compiler_params=pltpu.CompilerParams(collective_id=0, has_side_effects=True, vmem_limit_bytes=67_000_000),
            cost_estimate=pl.CostEstimate(flops=11 * flops, bytes_accessed=2**26, transcendentals=0),
        )(act_in.reshape(n_stage, rows, width), cot_out.reshape(n_stage, rows, width), w_gate, w_in, w_out)
        moved = sum(a.shape[0] for a in done)
        gg, gi, go, ga = pl.pallas_call(
            settle_kernel,
            name="settle",
            out_shape=results,
            in_specs=[hbm] * 4,
            out_specs=[hbm] * 4,
            scratch_shapes=[pltpu.VMEM(a.shape, a.dtype) for a in done] + [dma((moved,)), dma((moved,))],
        )(*done)
        return ga.reshape(act_in.shape), gg, gi, go

    return jax.shard_map(body, mesh=mesh, in_specs=(act_spec, act_spec, w_spec, w_spec, w_spec), out_specs=(act_spec, w_spec, w_spec, w_spec), check_vma=False)
```
